128 devices in a mesh: gx: 4 (over y), gy: 32 (over z, x, core).
Axes of the slice: x: 4, y: 4, z: 4, core: 2. Of those that a mesh axis runs over, the one named last changes fastest.
Arguments:
- background: float32 [256, 4, 512, 512], P(('gx', 'gy')), may hold values from -6 to 6
- obs_cells: int32 [32, 32, 1024], P('gy', 'gx'), may hold values from 0 to 2303
- obs_counts: int32 [32, 32], P('gy', 'gx'), may hold values from 1 to 1024, as said below
- obs_widths: int32 [32, 32], P('gy', 'gx'), may hold values from 1 to 4
- obs_values: float32 [32, 32, 1024], P('gy', 'gx'), may hold values from -6 to 6
- obs_variances: float32 [32, 32, 1024], P('gy', 'gx'), may hold values from 1 to 16
Outputs:
- analysis: float32 [256, 4, 512, 512], P(('gx', 'gy'))
The draws below stay inside these ranges and needn't reach their ends.
Inputs may be any that keep to these rules, and one draw needn't show every extreme that they name: `obs_cells`: each is level * 24 * 24 + row * 24 + column of a cell in the patch's surrounding region. `obs_counts`: some patch uses all 1024 slots.
All inputs are finite; a program needn't handle non-finite values.
Results may differ from the reference program's by a relative error of at most 0.0003.
Values sent between devices are 32-bit elements; how exact they have to be, the bound alone decides.
No kernel may reach another device: no remote copies, remote signals or barrier semaphores. Data moves between devices by JAX's collectives and lax.ppermute only.
A program may use at most 256 MiB of HBM per device.

```python
import math
import jax
import jax.numpy as jnp
from jax import lax

K = 256
LEV = 4
PSIDE = 16
HALO = 4
MAXOBS = 1024
ITERS = 5
PLAT = 32
PLON = 32
NLAT = 512
NLON = 512
AREA = 2304


def draw_obs_counts(key, part):
    latitude = lax.broadcasted_iota(jnp.int32, (PLAT, PLON), 0)
    polar = (latitude * 4 < PLAT) | (latitude * 4 >= 3 * PLAT)
    sparse = jax.random.randint(jax.random.fold_in(key, 11), (PLAT, PLON), 1, MAXOBS // 8 + 1)
    dense = jax.random.randint(jax.random.fold_in(key, 12), (PLAT, PLON), MAXOBS // 4, MAXOBS + 1)
    counts_all = jnp.where(polar, sparse, dense).reshape(-1)
    chosen = jax.random.randint(jax.random.fold_in(key, 13), (), 0, PLAT * PLON)
    counts_all = counts_all.at[chosen].set(MAXOBS)
    return counts_all.reshape(PLAT, PLON).astype(jnp.int32)


def place_ends(result, rng, low, top_value):
    longest = result.shape.index(max(result.shape))
    spots = []
    for shift in (0, 1):
        where = [jax.random.randint(jax.random.fold_in(rng, axis), (), 0, length) for axis, length in enumerate(result.shape)]
        where[longest] = (where[longest] + shift) % result.shape[longest]
        spots.append(tuple(where))
    return result.at[spots[0]].set(low).at[spots[1]].set(top_value)


def steps_of(stream_key, extent, shards, least, high):
    factor_of = 1.0
    for axis_at, shards_of in shards:
        draws = jax.random.uniform(jax.random.fold_in(jax.random.fold_in(stream_key, 6), axis_at), (shards_of,), jnp.float32, least / len(shards), high / len(shards))
        factor_of = factor_of * jnp.repeat(jnp.exp(draws), extent[axis_at] // shards_of).reshape((-1,) + (1,) * (len(extent) - 1 - axis_at))
    return factor_of


def scatter_about(own_key, dims, width, limit, cuts=(), held_as=jnp.bfloat16):
    values = jax.random.normal(own_key, dims, jnp.float32) * width
    if len(cuts) > 0:
        values = steps_of(own_key, dims, cuts, -0.22, 0.18) * values
    return jnp.clip(values, min=-limit, max=limit).astype(held_as)


def setup_inputs(seed: int = 0) -> dict:
    seeds = jax.random.split(jax.random.key(seed), 7)
    background = scatter_about(seeds[0], (K, LEV, NLAT, NLON), 1.0, 6.0, ((0, 128),), jnp.float32)
    obs_cells = place_ends(jax.random.randint(seeds[1], (PLAT, PLON, MAXOBS), 0, AREA), jax.random.fold_in(seeds[1], 1), 0, AREA - 1).astype(jnp.int32)
    obs_counts = draw_obs_counts(jax.random.fold_in(seeds[6], 71), 0)
    obs_widths = place_ends(jax.random.randint(seeds[3], (PLAT, PLON), 1, HALO + 1), jax.random.fold_in(seeds[3], 1), 1, HALO).astype(jnp.int32)
    obs_values = scatter_about(seeds[4], (PLAT, PLON, MAXOBS), 1.0, 6.0, ((0, 32), (1, 4)), jnp.float32)
    obs_variances = jnp.clip(jnp.exp(math.log(16.0) - 2.7725887 * jax.random.uniform(seeds[5], (PLAT, PLON, MAXOBS), jnp.float32) ** steps_of(seeds[5], (PLAT, PLON, MAXOBS), ((0, 32), (1, 4)), -0.2, 0.2)), 1.0, 16.0)
    return dict(background=background, obs_cells=obs_cells, obs_counts=obs_counts, obs_widths=obs_widths, obs_values=obs_values, obs_variances=obs_variances)


def product(former, latter):
    return jnp.einsum('nij,njk->nik', former, latter, precision=lax.Precision.HIGHEST)

def patches_of(region, core_side, margin):
    span_side = core_side + 2 * margin
    amount = (region.shape[3] - 2 * margin) // core_side
    pieces = [region[:, :, :, core_side * patch_index:core_side * patch_index + span_side] for patch_index in range(amount)]
    return jnp.stack(pieces, axis=0)

def observe(patches, obs_cells, obs_counts, obs_widths, obs_values, obs_variances, core_side, margin):
    number = patches.shape[0]
    ensemble_members = patches.shape[1]
    levels = patches.shape[2]
    span_side = patches.shape[3]
    flattened = patches.reshape(number, ensemble_members, levels * span_side * span_side)
    picker = jnp.broadcast_to(obs_cells[:, None, :], (number, ensemble_members, obs_cells.shape[1]))
    sampled = jnp.take_along_axis(flattened, picker, axis=2)
    sampled_mean = lax.optimization_barrier(jnp.mean(sampled, axis=1, keepdims=True))
    observed_spread = sampled - sampled_mean
    innovation = obs_values - sampled_mean[:, 0, :]
    row_pos = obs_cells // span_side % span_side
    col_pos = obs_cells % span_side
    row_out = jnp.maximum(jnp.maximum(margin - row_pos, row_pos - (margin + core_side - 1)), 0)
    col_out = jnp.maximum(jnp.maximum(margin - col_pos, col_pos - (margin + core_side - 1)), 0)
    distance = jnp.maximum(row_out, col_out)
    slot_ids = lax.broadcasted_iota(jnp.int32, obs_cells.shape, 1)
    usable = (slot_ids < obs_counts[:, None]) & (distance <= obs_widths[:, None])
    relative = distance.astype(jnp.float32) / (obs_widths[:, None] + 1).astype(jnp.float32)
    weights = jnp.where(usable, jnp.exp(-relative * relative) / obs_variances, 0.0)
    scaled_spread = observed_spread * weights[:, None, :]
    pulled = lax.optimization_barrier(jnp.sum(scaled_spread * innovation[:, None, :], axis=2))
    return (scaled_spread, observed_spread, pulled)

def settle(gram_sum, pulled, patches, core_side, margin, sweeps):
    ensemble_members = gram_sum.shape[1]
    identity_m = jnp.eye(ensemble_members, dtype=jnp.float32)
    frobenius = jnp.sqrt(lax.optimization_barrier(jnp.sum(gram_sum * gram_sum, axis=(1, 2))))
    divisor = ensemble_members - 1.0 + frobenius
    current = (gram_sum + (ensemble_members - 1.0) * identity_m) / divisor[:, None, None]
    inverse_root = jnp.broadcast_to(identity_m, gram_sum.shape)
    for repeat in range(sweeps):
        factor = 1.5 * identity_m - 0.5 * product(inverse_root, current)
        current = product(current, factor)
        inverse_root = product(factor, inverse_root)
    halfway = jnp.einsum('nkj,nj->nk', inverse_root, pulled, precision=lax.Precision.HIGHEST)
    mean_weight = jnp.einsum('nkj,nj->nk', inverse_root, halfway, precision=lax.Precision.HIGHEST) / divisor[:, None]
    combined = jnp.sqrt((ensemble_members - 1.0) / divisor)[:, None, None] * inverse_root + mean_weight[:, :, None]
    core_cells = patches[:, :, :, margin:margin + core_side, margin:margin + core_side]
    patch_centre = lax.optimization_barrier(jnp.mean(core_cells, axis=1, keepdims=True))
    deviation = core_cells - patch_centre
    return patch_centre + jnp.einsum('njk,njlab->nklab', combined, deviation, precision=lax.Precision.HIGHEST)

def assemble(analysed):
    number = analysed.shape[0]
    ensemble_members = analysed.shape[1]
    levels = analysed.shape[2]
    core_side = analysed.shape[3]
    moved = jnp.transpose(analysed, (1, 2, 3, 0, 4))
    return moved.reshape(ensemble_members, levels, core_side, number * core_side)

def reference(background, obs_cells, obs_counts, obs_widths, obs_values, obs_variances):
    padded_state = jnp.pad(background, ((0, 0), (0, 0), (HALO, HALO), (0, 0)))
    padded_state = jnp.concatenate([padded_state[:, :, :, -HALO:], padded_state, padded_state[:, :, :, :HALO]], axis=3)

    def one_band(packed_state):
        band_index, band_cells, band_counts, band_widths, band_values, band_variances = packed_state
        region = lax.dynamic_slice_in_dim(padded_state, band_index * PSIDE, PSIDE + 2 * HALO, 2)
        patches = patches_of(region, PSIDE, HALO)
        scaled_spread, observed_spread, pulled = observe(patches, band_cells, band_counts, band_widths, band_values, band_variances, PSIDE, HALO)
        gram_sum = jnp.einsum('nkm,njm->nkj', scaled_spread, observed_spread, precision=lax.Precision.HIGHEST)
        return assemble(settle(gram_sum, pulled, patches, PSIDE, HALO, ITERS))
    bands = lax.map(one_band, (jnp.arange(PLAT, dtype=jnp.int32), obs_cells, obs_counts, obs_widths, obs_values, obs_variances))
    return jnp.transpose(bands, (1, 2, 0, 3, 4)).reshape(K, LEV, NLAT, NLON)
```

```python
import functools

import jax
import jax.numpy as jnp
from jax import lax
from jax.experimental import pallas as pl
from jax.experimental.pallas import tpu as pltpu
from jax.sharding import PartitionSpec as P

F32 = jnp.float32
BF16 = jnp.bfloat16
ITERS = 5
FIRST, SECOND = (1,), (3, 5, 7)
CORE_ROWS = 8
ALL_ROWS = 12


def lane_group(shape):
    return lax.broadcasted_iota(jnp.int32, shape, len(shape) - 1) // 16


def skew(tiles):
    group = lane_group(tiles[0].shape)
    for bit in (1, 2, 4):
        odd = (group & bit) != 0
        tiles = [jnp.where(odd, tiles[(k + bit) % 8], tiles[k]) for k in range(8)]
    return tiles


def pack_kernel(x_ref, o_ref):
    bands = o_ref.shape[1]
    for band in range(bands):
        for member in range(2):
            for col in range(4):
                tiles = []
                for t in range(8):
                    row = 16 * band + 8 * (t % 2)
                    tile = x_ref[member, t // 2, row : row + 8, 128 * col : 128 * col + 128]
                    tiles.append(pltpu.roll(tile, 16 * t, 1) if t else tile)
                tiles = skew(tiles)
                for p in range(8):
                    o_ref[col, band, member, 8 * p : 8 * p + 8, :] = tiles[(8 - p) % 8]


def pack(x, bands=2):
    return pl.pallas_call(
        pack_kernel,
        grid=(32 // bands,),
        in_specs=[pl.BlockSpec((2, 4, 16 * bands, 512), lambda i: (0, 0, i, 0))],
        out_specs=pl.BlockSpec((4, bands, 2, 64, 128), lambda i: (0, i, 0, 0, 0)),
        out_shape=jax.ShapeDtypeStruct((4, 32, 2, 64, 128), F32),
        name="pack",
    )(x)


def unpack_kernel(a_ref, b_ref, o_ref, *, order):
    bands = a_ref.shape[1]
    place = {p: (a_ref, i) for i, p in enumerate(order[0])}
    place.update({p: (b_ref, i) for i, p in enumerate(order[1])})
    for band in range(bands):
        for member in range(2):
            for col in range(4):
                tiles = []
                for p in range(8):
                    ref, i = place[p]
                    tiles.append(ref[col, band, member, 8 * i : 8 * i + 8, :])
                tiles = skew(tiles)
                for t in range(8):
                    tile = tiles[(8 - t) % 8]
                    tile = pltpu.roll(tile, 128 - 16 * t, 1) if t else tile
                    row = 16 * band + 8 * (t % 2)
                    o_ref[member, t // 2, row : row + 8, 128 * col : 128 * col + 128] = tile


def unpack(a, b, order, bands=2):
    na, nb = 8 * len(order[0]), 8 * len(order[1])
    return pl.pallas_call(
        functools.partial(unpack_kernel, order=order),
        grid=(32 // bands,),
        in_specs=[
            pl.BlockSpec((4, bands, 2, na, 128), lambda i: (0, i, 0, 0, 0)),
            pl.BlockSpec((4, bands, 2, nb, 128), lambda i: (0, i, 0, 0, 0)),
        ],
        out_specs=pl.BlockSpec((2, 4, 16 * bands, 512), lambda i: (0, 0, i, 0)),
        out_shape=jax.ShapeDtypeStruct((2, 4, 512, 512), F32),
        name="unpack",
    )(a, b)


def three_way(x):
    high = x.astype(BF16)
    rest = x - high.astype(F32)
    mid = rest.astype(BF16)
    return high, mid, (rest - mid.astype(F32)).astype(BF16)


def two_way(x):
    high = x.astype(BF16)
    return high, (x - high.astype(F32)).astype(BF16)


def cells_kernel(kc_ref, lane_ref, w_ref, v_ref, o_ref):
    kc = kc_ref[0]
    slots = kc.shape[1]
    row_hit = lax.broadcasted_iota(jnp.int32, (24, slots), 0) == kc
    lane_hit = lax.broadcasted_iota(jnp.int32, (128, slots), 0) == lane_ref[0]
    lane_hot = jnp.where(lane_hit, 1.0, 0.0).astype(BF16)
    both = jnp.concatenate(
        [jnp.where(row_hit, w_ref[0], 0.0), jnp.where(row_hit, v_ref[0], 0.0)], axis=0
    )
    total = jnp.zeros((48, 128), F32)
    for part in three_way(both):
        total = total + lax.dot_general(
            part, lane_hot, (((1,), (1,)), ((), ())), preferred_element_type=F32
        )
    w = total[:24]
    root = jnp.where(w > 0.0, jnp.sqrt(jnp.maximum(w, 1e-30)), 0.0)
    o_ref[0] = jnp.concatenate([total, root], axis=0)


def cell_sums(obs_cells, obs_counts, obs_widths, obs_values, obs_variances):
    number, slots = obs_cells.shape
    level = obs_cells // 576
    row = obs_cells // 24 % 24
    col = obs_cells % 24
    row_out = jnp.maximum(jnp.maximum(4 - row, row - 19), 0)
    col_out = jnp.maximum(jnp.maximum(4 - col, col - 19), 0)
    distance = jnp.maximum(row_out, col_out)
    slot = lax.broadcasted_iota(jnp.int32, obs_cells.shape, 1)
    usable = (slot < obs_counts[:, None]) & (distance <= obs_widths[:, None])
    relative = distance.astype(F32) / (obs_widths[:, None] + 1).astype(F32)
    w = jnp.where(usable, jnp.exp(-relative * relative) / obs_variances, 0.0)
    v = w * obs_values
    own = (row >= 4) & (row < 20)
    above = row < 4
    t = 2 * level + jnp.where(own, (row - 4) // 8, jnp.where(above, 1, 0))
    q = jnp.where(own, (row - 4) % 8, 8 + jnp.where(above, row, row - 20))
    west, east = col < 4, col >= 20
    shift = jnp.where(west, -1, jnp.where(east, 1, 0))
    inner = jnp.where(west, 12 + col, jnp.where(east, col - 20, col - 4))
    p = lax.broadcasted_iota(jnp.int32, obs_cells.shape, 0)
    lane = 16 * ((t + p + shift + 8) % 8) + inner
    kc = q + jnp.where(west | east, ALL_ROWS, 0)
    spec = pl.BlockSpec((1, 1, slots), lambda i: (i, 0, 0))
    shape = (number, 1, slots)
    return pl.pallas_call(
        cells_kernel,
        grid=(number,),
        in_specs=[spec] * 4,
        out_specs=pl.BlockSpec((1, 72, 128), lambda i: (i, 0, 0)),
        out_shape=jax.ShapeDtypeStruct((number, 72, 128), F32),
        name="cells",
    )(kc.reshape(shape), lane.reshape(shape), w.reshape(shape), v.reshape(shape))


def edges_kernel(x_ref, up_ref, dn_ref):
    shape = (1, 8, 128)
    low = lax.broadcasted_iota(jnp.int32, shape, 1) < 4
    even = lane_group(shape) % 2 == 0
    first = even == low
    for i in range(4):
        a = x_ref[:, 16 * i : 16 * i + 8, :]
        b = x_ref[:, 16 * i + 8 : 16 * i + 16, :]
        merged = jnp.where(first, a, b)
        up_ref[:, 4 * i : 4 * i + 4, :] = merged[:, 0:4, :]
        dn_ref[:, 4 * i : 4 * i + 4, :] = merged[:, 4:8, :]


def edges(x, members=32):
    shape = jax.ShapeDtypeStruct((256, 16, 128), F32)
    spec = pl.BlockSpec((members, 16, 128), lambda i: (i, 0, 0))
    return pl.pallas_call(
        edges_kernel,
        grid=(256 // members,),
        in_specs=[pl.BlockSpec((members, 64, 128), lambda i: (i, 0, 0))],
        out_specs=[spec, spec],
        out_shape=[shape, shape],
        name="edges",
    )(x)


def take(ref, row):
    members, rows, lanes = ref.shape
    return ref.reshape(members * rows, lanes)[pl.ds(row, members, stride=rows), :]


def put(ref, row, value):
    members, rows, lanes = ref.shape
    ref.reshape(members * rows, lanes)[pl.ds(row, members, stride=rows), :] = value


def rows_of(block, above, below, p, q):
    if q < CORE_ROWS:
        return take(block, q)
    start = (p // 2) * 4 + (q - CORE_ROWS)
    a = take(above, start)
    b = take(below, start)
    return jnp.where(((lane_group((1, 128)) - p) & 1) == 1, a, b)


def sides_kernel(first_ref, last_ref, above_ref, below_ref, left_ref, right_ref):
    within = lax.broadcasted_iota(jnp.int32, (1, 128), 1) % 16 // 4
    for j in range(3):
        left = right = None
        for i in range(4):
            f = rows_of(first_ref, above_ref, below_ref, 0, 4 * j + i)
            f = pltpu.roll(f, 4 * i, 1) if i else f
            l = rows_of(last_ref, above_ref, below_ref, 7, 4 * j + i)
            l = pltpu.roll(l, 128 - 4 * (3 - i), 1) if i < 3 else l
            left = f if left is None else jnp.where(within == i, f, left)
            right = l if right is None else jnp.where(within == i, l, right)
        left_ref[:, 128 * j : 128 * j + 128] = left
        right_ref[:, 128 * j : 128 * j + 128] = right


def sides(x, above, below):
    shape = jax.ShapeDtypeStruct((256, 384), F32)
    whole = pl.BlockSpec((256, 16, 128), lambda i: (0, 0, 0))
    return pl.pallas_call(
        sides_kernel,
        grid=(1,),
        in_specs=[
            pl.BlockSpec((256, 8, 128), lambda i: (0, 0, 0)),
            pl.BlockSpec((256, 8, 128), lambda i: (0, 7, 0)),
            whole,
            whole,
        ],
        out_specs=[pl.BlockSpec((256, 384), lambda i: (0, 0))] * 2,
        out_shape=[shape, shape],
        name="sides",
    )(x, x, above, below)


def dot(a, b):
    return jnp.dot(a, b, preferred_element_type=F32)


def product(a, b):
    (ah, al), (bh, bl) = a, b
    return dot(jnp.concatenate([ah, ah, al], axis=1), jnp.concatenate([bh, bl, bh], axis=0))


def analyse(p, west, mine, east, above, below, strips, wv, out, base, high_ref, low_ref, gram_ref):
    total = jnp.zeros((256, 128), F32)
    within = lax.broadcasted_iota(jnp.int32, (1, 128), 1) % 16
    for c in range(2 * ALL_ROWS):
        q = c % ALL_ROWS
        if c < ALL_ROWS:
            x = rows_of(mine, above, below, p, q)
        else:
            l = rows_of(west, above, below, (p + 7) % 8, q)
            r = rows_of(east, above, below, (p + 1) % 8, q)
            if strips is not None:
                first, last = strips
                i, j = q % 4, q // 4
                if first is not None:
                    far = first[:, 128 * j : 128 * j + 128]
                    far = pltpu.roll(far, 4 * (3 - i), 1) if i < 3 else far
                    l = jnp.where(p == 0, far, l)
                if last is not None:
                    far = last[:, 128 * j : 128 * j + 128]
                    far = pltpu.roll(far, 128 - 4 * i, 1) if i else far
                    r = jnp.where(p == 7, far, r)
            x = jnp.where(within < 8, r, l)
        w = wv[0, c : c + 1, :]
        v = wv[0, 24 + c : 25 + c, :]
        root = wv[0, 48 + c : 49 + c, :]
        mean = jnp.sum(x, axis=0, keepdims=True) * (1.0 / 256)
        dev = x - mean
        total = total + dev * (v - w * mean)
        high, low = two_way(dev * root)
        high_ref[:, 128 * c : 128 * c + 128] = high
        low_ref[:, 128 * c : 128 * c + 128] = low
    nt = (((1,), (1,)), ((), ()))
    gram_ref[0] = lax.dot_general(high_ref[...], high_ref[...], nt, preferred_element_type=F32)
    gram_ref[1] = lax.dot_general(high_ref[...], low_ref[...], nt, preferred_element_type=F32)
    cross = gram_ref[1]
    gram = gram_ref[0] + (cross + cross.T)
    pulled = jnp.sum(total, axis=1, keepdims=True)

    squares = jnp.sum(jnp.sum(gram * gram, axis=0, keepdims=True), axis=1, keepdims=True)
    divisor = 255.0 + jnp.sqrt(jnp.maximum(squares, 1e-30))
    row = lax.broadcasted_iota(jnp.int32, (256, 256), 0)
    col = lax.broadcasted_iota(jnp.int32, (256, 256), 1)
    eye = row == col
    current = (gram + jnp.where(eye, 255.0, 0.0)) / divisor
    inverse = jnp.where(eye, 1.5, 0.0) - 0.5 * current
    current = product(two_way(current), two_way(inverse))
    for step in range(1, ITERS):
        cur, inv = two_way(current), two_way(inverse)
        factor = two_way(jnp.where(eye, 1.5, 0.0) - 0.5 * product(inv, cur))
        if step < ITERS - 1:
            current = product(cur, factor)
        inverse = product(factor, inv)
    halfway = jnp.sum(inverse * pulled, axis=0, keepdims=True)
    weight = jnp.sum(inverse * halfway, axis=1, keepdims=True) / divisor
    zh, zl = two_way(inverse * jnp.sqrt(255.0 / divisor))
    z = jnp.concatenate([zh, zh, zl], axis=1)
    for q in range(0, CORE_ROWS, 2):
        parts, bases = [], []
        for k in range(2):
            x = rows_of(mine, above, below, p, q + k)
            centre = jnp.sum(x, axis=0, keepdims=True) * (1.0 / 256)
            dev = x - centre
            bases.append(centre + jnp.sum(dev * weight, axis=0, keepdims=True))
            parts.append(dev)
        dh, dl = two_way(jnp.concatenate(parts, axis=1))
        mixed = dot(z, jnp.concatenate([dh, dl, dh], axis=0))
        for k in range(2):
            o = mixed[:, 128 * k : 128 * k + 128] + bases[k]
            put(out, base + q + k, o)


def analysis_kernel(pairs, with_sides, *refs):
    x0, x1, x2, x3, above, below = refs[:6]
    refs = refs[6:]
    strips = [None, None]
    if with_sides:
        strips = [(None, refs[1]), (refs[0], None)]
        refs = refs[2:]
    wv0, wv1, out, h0, l0, h1, l1, g0, g1 = refs
    p = pairs[0] + 2 * pl.program_id(0)
    analyse(p, x0, x1, x2, above, below, strips[0], wv0, out, 0, h0, l0, g0)
    analyse((p + 1) % 8, x1, x2, x3, above, below, strips[1], wv1, out, 8, h1, l1, g1)


def analysis(x, above, below, left, right, wv, pairs):
    with_sides = pairs[-1] == 7
    steps = len(pairs)
    start = pairs[0]

    def block(shift):
        return pl.BlockSpec((256, 8, 128), lambda i: (0, (start + 2 * i + shift + 8) % 8, 0))

    def cells(shift):
        return pl.BlockSpec((1, 72, 128), lambda i: ((start + 2 * i + shift) % 8, 0, 0))

    whole = pl.BlockSpec((256, 16, 128), lambda i: (0, 0, 0))
    side = pl.BlockSpec((256, 384), lambda i: (0, 0))
    args = [x, x, x, x, above, below]
    specs = [block(-1), block(0), block(1), block(2), whole, whole]
    if with_sides:
        args += [left, right]
        specs += [side, side]
    args += [wv, wv]
    specs += [cells(0), cells(1)]
    return pl.pallas_call(
        functools.partial(analysis_kernel, pairs, with_sides),
        grid=(steps,),
        in_specs=specs,
        out_specs=pl.BlockSpec((256, 16, 128), lambda i: (0, i, 0)),
        out_shape=jax.ShapeDtypeStruct((256, 16 * steps, 128), F32),
        scratch_shapes=[pltpu.VMEM((256, 24 * 128), BF16)] * 4
        + [pltpu.VMEM((2, 256, 256), F32)] * 2,
        compiler_params=pltpu.CompilerParams(vmem_limit_bytes=60000 * 1024),
        cost_estimate=pl.CostEstimate(
            flops=steps * 2 * 72 * 2 * 256**3, bytes_accessed=steps * 12 * 2**20, transcendentals=0
        ),
        name="analysis",
    )(*args)


def shards(background, obs_cells, obs_counts, obs_widths, obs_values, obs_variances):
    axes = ("gx", "gy")
    gx, gy = lax.axis_size("gx"), lax.axis_size("gy")
    send = pack(background).reshape(256, 64, 128)
    x = lax.all_to_all(send, axes, split_axis=0, concat_axis=0, tiled=True)
    wv = cell_sums(obs_cells[0], obs_counts[0], obs_widths[0], obs_values[0], obs_variances[0])
    up, dn = edges(x)
    onward = [(i, i + 1) for i in range(gy - 1)]
    above = lax.ppermute(dn, "gy", onward)
    below = lax.ppermute(up, "gy", [(j, i) for i, j in onward])
    to_left, to_right = sides(x, above, below)
    ring = [(i, (i + 1) % gx) for i in range(gx)]
    left = lax.ppermute(to_right, "gx", ring)
    right = lax.ppermute(to_left, "gx", [(j, i) for i, j in ring])
    results, order = [], []
    for pairs in (FIRST, SECOND):
        out = analysis(x, above, below, left, right, wv, pairs)
        results.append(lax.all_to_all(out, axes, split_axis=0, concat_axis=0, tiled=True))
        order.append([q % 8 for p in pairs for q in (p, p + 1)])
    a, b = [r.reshape(4, 32, 2, r.shape[1], 128) for r in results]
    return unpack(a, b, order)


def solution(mesh):
    return jax.shard_map(
        shards,
        mesh=mesh,
        in_specs=(
            P(("gx", "gy"), None, None, None),
            P("gy", "gx", None),
            P("gy", "gx"),
            P("gy", "gx"),
            P("gy", "gx", None),
            P("gy", "gx", None),
        ),
        out_specs=P(("gx", "gy"), None, None, None),
        check_vma=False,
    )
```

```python
import functools

import jax
import jax.numpy as jnp
from jax import lax
from jax.experimental import pallas as pl
from jax.experimental.pallas import tpu as pltpu
from jax.sharding import PartitionSpec as P

F32 = jnp.float32
BF16 = jnp.bfloat16
ITERS = 5
FIRST, SECOND = (1,), (3, 5, 7)


def lane_group(shape):
    return lax.broadcasted_iota(jnp.int32, shape, len(shape) - 1) // 16


def skew(tiles):
    group = lane_group(tiles[0].shape)
    for bit in (1, 2, 4):
        odd = (group & bit) != 0
        tiles = [jnp.where(odd, tiles[(k + bit) % 8], tiles[k]) for k in range(8)]
    return tiles


def edge_lanes():
    shape = (8, 128)
    low = lax.broadcasted_iota(jnp.int32, shape, 0) < 4
    return (lane_group(shape) % 2 == 0) == low


def pack_kernel(x_ref, o_ref, *, edge):
    bands = o_ref.shape[1]
    first = edge_lanes()
    for band in range(bands):
        for member in range(2):
            for col in range(4):
                tiles = []
                for t in range(8):
                    row = 16 * band + 8 * (t % 2)
                    tile = x_ref[member, t // 2, row : row + 8, 128 * col : 128 * col + 128]
                    tiles.append(pltpu.roll(tile, 16 * t, 1) if t else tile)
                tiles = skew(tiles)
                for i in range(4):
                    even, odd = tiles[(8 - 2 * i) % 8], tiles[7 - 2 * i]
                    merged = jnp.where(first, even, odd) if edge else jnp.where(first, odd, even)
                    o_ref[col, band, member, 8 * i : 8 * i + 8, :] = merged


def pack(x, edge, bands=2):
    return pl.pallas_call(
        functools.partial(pack_kernel, edge=edge),
        grid=(32 // bands,),
        in_specs=[pl.BlockSpec((2, 4, 16 * bands, 512), lambda i: (0, 0, i, 0))],
        out_specs=pl.BlockSpec((4, bands, 2, 32, 128), lambda i: (0, i, 0, 0, 0)),
        out_shape=jax.ShapeDtypeStruct((4, 32, 2, 32, 128), F32),
        cost_estimate=pl.CostEstimate(flops=10**10, bytes_accessed=12 * 2**20, transcendentals=0),
        name="pack_edge" if edge else "pack_inner",
    )(x)


def unpack_kernel(a_ref, b_ref, o_ref, *, order):
    bands = a_ref.shape[1]
    place = {p: (a_ref, i) for i, p in enumerate(order[0])}
    place.update({p: (b_ref, i) for i, p in enumerate(order[1])})
    for band in range(bands):
        for member in range(2):
            for col in range(4):
                tiles = []
                for p in range(8):
                    ref, i = place[p]
                    tiles.append(ref[col, band, member, 8 * i : 8 * i + 8, :])
                tiles = skew(tiles)
                for t in range(8):
                    tile = tiles[(8 - t) % 8]
                    tile = pltpu.roll(tile, 128 - 16 * t, 1) if t else tile
                    row = 16 * band + 8 * (t % 2)
                    o_ref[member, t // 2, row : row + 8, 128 * col : 128 * col + 128] = tile


def unpack(a, b, order, bands=2):
    na, nb = 8 * len(order[0]), 8 * len(order[1])
    return pl.pallas_call(
        functools.partial(unpack_kernel, order=order),
        grid=(32 // bands,),
        in_specs=[
            pl.BlockSpec((4, bands, 2, na, 128), lambda i: (0, i, 0, 0, 0)),
            pl.BlockSpec((4, bands, 2, nb, 128), lambda i: (0, i, 0, 0, 0)),
        ],
        out_specs=pl.BlockSpec((2, 4, 16 * bands, 512), lambda i: (0, 0, i, 0)),
        out_shape=jax.ShapeDtypeStruct((2, 4, 512, 512), F32),
        name="unpack",
    )(a, b)


def three_way(x):
    high = x.astype(BF16)
    rest = x - high.astype(F32)
    mid = rest.astype(BF16)
    return high, mid, (rest - mid.astype(F32)).astype(BF16)


def two_way(x):
    high = x.astype(BF16)
    return high, (x - high.astype(F32)).astype(BF16)


def cells_kernel(kc_ref, lane_ref, w_ref, v_ref, o_ref):
    kc = kc_ref[0]
    slots = kc.shape[1]
    row_hit = lax.broadcasted_iota(jnp.int32, (24, slots), 0) == kc
    lane_hit = lax.broadcasted_iota(jnp.int32, (128, slots), 0) == lane_ref[0]
    lane_hot = jnp.where(lane_hit, 1.0, 0.0).astype(BF16)
    both = jnp.concatenate(
        [jnp.where(row_hit, w_ref[0], 0.0), jnp.where(row_hit, v_ref[0], 0.0)], axis=0
    )
    total = jnp.zeros((48, 128), F32)
    for part in three_way(both):
        total = total + lax.dot_general(
            part, lane_hot, (((1,), (1,)), ((), ())), preferred_element_type=F32
        )
    w = total[:24]
    root = jnp.where(w > 0.0, jnp.sqrt(jnp.maximum(w, 1e-30)), 0.0)
    o_ref[0] = jnp.concatenate([total, root], axis=0)


def cell_sums(obs_cells, obs_counts, obs_widths, obs_values, obs_variances):
    number, slots = obs_cells.shape
    level = obs_cells // 576
    row = obs_cells // 24 % 24
    col = obs_cells % 24
    row_out = jnp.maximum(jnp.maximum(4 - row, row - 19), 0)
    col_out = jnp.maximum(jnp.maximum(4 - col, col - 19), 0)
    distance = jnp.maximum(row_out, col_out)
    slot = lax.broadcasted_iota(jnp.int32, obs_cells.shape, 1)
    usable = (slot < obs_counts[:, None]) & (distance <= obs_widths[:, None])
    relative = distance.astype(F32) / (obs_widths[:, None] + 1).astype(F32)
    w = jnp.where(usable, jnp.exp(-relative * relative) / obs_variances, 0.0)
    v = w * obs_values
    t = 2 * level + jnp.where((row >= 12) & (row < 20) | (row < 4), 1, 0)
    halo = (row < 4) | (row >= 20)
    inside = (row >= 8) & (row < 16)
    west, east = col < 4, col >= 20
    shift = jnp.where(west, -1, jnp.where(east, 1, 0))
    inner = jnp.where(west, 12 + col, jnp.where(east, col - 20, col - 4))
    p = lax.broadcasted_iota(jnp.int32, obs_cells.shape, 0)
    lane = 16 * ((t + p + shift + 8) % 8) + inner
    side = jnp.where(west | east, 1, 0)
    kc = row % 4 + jnp.where(inside, 16 + 4 * side, 8 * side + jnp.where(halo, 4, 0))
    spec = pl.BlockSpec((1, 1, slots), lambda i: (i, 0, 0))
    shape = (number, 1, slots)
    return pl.pallas_call(
        cells_kernel,
        grid=(number,),
        in_specs=[spec] * 4,
        out_specs=pl.BlockSpec((1, 72, 128), lambda i: (i, 0, 0)),
        out_shape=jax.ShapeDtypeStruct((number, 72, 128), F32),
        cost_estimate=pl.CostEstimate(flops=5 * 10**9, bytes_accessed=2**20, transcendentals=0),
        name="cells",
    )(kc.reshape(shape), lane.reshape(shape), w.reshape(shape), v.reshape(shape))


def take(ref, row):
    members, rows, lanes = ref.shape
    return ref.reshape(members * rows, lanes)[pl.ds(row, members, stride=rows), :]


def put(ref, row, value):
    members, rows, lanes = ref.shape
    ref.reshape(members * rows, lanes)[pl.ds(row, members, stride=rows), :] = value


def odd_rows(odd):
    return ((lane_group((1, 128)) - odd) & 1) == 1


def column(kind, q, patch, above, below):
    edge, inner, pair, odd = patch
    if kind == "edge":
        a, b = take(edge, q), take(edge, 4 + q)
    elif kind == "inner":
        a, b = take(inner, 4 + q), take(inner, q)
    else:
        a, b = take(below, 4 * pair + q), take(above, 4 * pair + q)
    return jnp.where(odd_rows(odd), b, a)


def sides_kernel(*refs, kinds):
    count = len(kinds)
    first_ref, last_ref = refs[:2]
    above, below = refs[2:4] if "halo" in kinds else (None, None)
    left_ref, right_ref = refs[-2:]
    within = lax.broadcasted_iota(jnp.int32, (1, 128), 1) % 16 // 4
    for j in range(count):
        left = right = None
        for i in range(4):
            f = column(kinds[j], i, (first_ref, first_ref, 0, 0), above, below)
            f = pltpu.roll(f, 4 * i, 1) if i else f
            l = column(kinds[j], i, (last_ref, last_ref, 3, 1), above, below)
            l = pltpu.roll(l, 128 - 4 * (3 - i), 1) if i < 3 else l
            left = f if left is None else jnp.where(within == i, f, left)
            right = l if right is None else jnp.where(within == i, l, right)
        left_ref[:, 128 * j : 128 * j + 128] = left
        right_ref[:, 128 * j : 128 * j + 128] = right


def whole(shape):
    return pl.BlockSpec(shape, lambda i: (0,) * len(shape))


def sides(x, kinds, *halo):
    width = 128 * len(kinds)
    return pl.pallas_call(
        functools.partial(sides_kernel, kinds=kinds),
        grid=(1,),
        in_specs=[
            pl.BlockSpec((256, 8, 128), lambda i: (0, 0, 0)),
            pl.BlockSpec((256, 8, 128), lambda i: (0, 3, 0)),
        ]
        + [whole((256, 16, 128))] * len(halo),
        out_specs=[whole((256, width))] * 2,
        out_shape=[jax.ShapeDtypeStruct((256, width), F32)] * 2,
        cost_estimate=pl.CostEstimate(flops=10**9, bytes_accessed=4 * 2**20, transcendentals=0),
        name="sides",
    )(x, x, *halo)


def dot(a, b):
    return jnp.dot(a, b, preferred_element_type=F32)


def product(a, b):
    (ah, al), (bh, bl) = a, b
    return dot(jnp.concatenate([ah, ah, al], axis=1), jnp.concatenate([bh, bl, bh], axis=0))


def gram_of(kinds, base, west, mine, east, above, below, far, wv, high_ref, low_ref, gram_ref):
    total = jnp.zeros((256, 128), F32)
    within = lax.broadcasted_iota(jnp.int32, (1, 128), 1) % 16
    place = 0
    for strip in (False, True):
        for j, kind in enumerate(kinds):
            for q in range(4):
                if not strip:
                    x = column(kind, q, mine, above, below)
                else:
                    l = column(kind, q, west, above, below)
                    r = column(kind, q, east, above, below)
                    if far is not None:
                        ref, from_west, outer = far
                        v = ref[:, 128 * j : 128 * j + 128]
                        if from_west:
                            v = pltpu.roll(v, 4 * (3 - q), 1) if q < 3 else v
                            l = jnp.where(outer, v, l)
                        else:
                            v = pltpu.roll(v, 128 - 4 * q, 1) if q else v
                            r = jnp.where(outer, v, r)
                    x = jnp.where(within < 8, r, l)
                c = base + place
                w = wv[0, c : c + 1, :]
                v = wv[0, 24 + c : 25 + c, :]
                root = wv[0, 48 + c : 49 + c, :]
                mean = jnp.sum(x, axis=0, keepdims=True) * (1.0 / 256)
                dev = x - mean
                total = total + dev * (v - w * mean)
                high, low = two_way(dev * root)
                high_ref[:, 128 * place : 128 * place + 128] = high
                low_ref[:, 128 * place : 128 * place + 128] = low
                place += 1
    nt = (((1,), (1,)), ((), ()))
    high, low = high_ref[:, : 128 * place], low_ref[:, : 128 * place]
    gram_ref[0] = lax.dot_general(high, high, nt, preferred_element_type=F32)
    gram_ref[1] = lax.dot_general(high, low, nt, preferred_element_type=F32)
    cross = gram_ref[1]
    return gram_ref[0] + (cross + cross.T), total


def early_kernel(e0, e1, above, below, wv0, wv1, gram_out, pulled_out, h0, l0, h1, l1, g0, g1):
    pair = pl.program_id(0)
    patches = [(e, None, pair + i // 2, i % 2) for i, e in enumerate((e0, e0, e1, e1))]
    for k, wv, h, l, g in ((0, wv0, h0, l0, g0), (1, wv1, h1, l1, g1)):
        gram, total = gram_of(
            ("edge", "halo"), 0, *patches[k : k + 3], above, below, None, wv, h, l, g
        )
        gram_out[k] = gram
        pulled_out[k] = total


def early(edge, above, below, wv):
    steps = 3
    return pl.pallas_call(
        early_kernel,
        grid=(steps,),
        in_specs=[
            pl.BlockSpec((256, 8, 128), lambda i: (0, i, 0)),
            pl.BlockSpec((256, 8, 128), lambda i: (0, i + 1, 0)),
            whole((256, 16, 128)),
            whole((256, 16, 128)),
            pl.BlockSpec((1, 72, 128), lambda i: (2 * i + 1, 0, 0)),
            pl.BlockSpec((1, 72, 128), lambda i: (2 * i + 2, 0, 0)),
        ],
        out_specs=[
            pl.BlockSpec((2, 256, 256), lambda i: (i, 0, 0)),
            pl.BlockSpec((2, 256, 128), lambda i: (i, 0, 0)),
        ],
        out_shape=[
            jax.ShapeDtypeStruct((6, 256, 256), F32),
            jax.ShapeDtypeStruct((6, 256, 128), F32),
        ],
        scratch_shapes=[pltpu.VMEM((256, 2048), BF16)] * 4 + [pltpu.VMEM((2, 256, 256), F32)] * 2,
        compiler_params=pltpu.CompilerParams(vmem_limit_bytes=60000 * 1024),
        cost_estimate=pl.CostEstimate(
            flops=20 * 10**9, bytes_accessed=12 * 2**20, transcendentals=0
        ),
        name="early",
    )(edge, edge, above, below, wv, wv)


def analyse(gram, total, mine, out, base):
    pulled = jnp.sum(total, axis=1, keepdims=True)
    squares = jnp.sum(jnp.sum(gram * gram, axis=0, keepdims=True), axis=1, keepdims=True)
    divisor = 255.0 + jnp.sqrt(jnp.maximum(squares, 1e-30))
    row = lax.broadcasted_iota(jnp.int32, (256, 256), 0)
    col = lax.broadcasted_iota(jnp.int32, (256, 256), 1)
    eye = row == col
    current = (gram + jnp.where(eye, 255.0, 0.0)) / divisor
    inverse = jnp.where(eye, 1.5, 0.0) - 0.5 * current
    current = product(two_way(current), two_way(inverse))
    for step in range(1, ITERS):
        cur, inv = two_way(current), two_way(inverse)
        factor = two_way(jnp.where(eye, 1.5, 0.0) - 0.5 * product(inv, cur))
        if step < ITERS - 1:
            current = product(cur, factor)
        inverse = product(factor, inv)
    halfway = jnp.sum(inverse * pulled, axis=0, keepdims=True)
    weight = jnp.sum(inverse * halfway, axis=1, keepdims=True) / divisor
    zh, zl = two_way(inverse * jnp.sqrt(255.0 / divisor))
    z = jnp.concatenate([zh, zh, zl], axis=1)
    edge, inner, _, odd = mine
    for q in range(0, 8, 2):
        parts, bases = [], []
        for k in range(2):
            a, b = take(edge, q + k), take(inner, q + k)
            x = jnp.where(odd_rows(odd), b, a) if q < 4 else jnp.where(odd_rows(odd), a, b)
            centre = jnp.sum(x, axis=0, keepdims=True) * (1.0 / 256)
            dev = x - centre
            bases.append(centre + jnp.sum(dev * weight, axis=0, keepdims=True))
            parts.append(dev)
        dh, dl = two_way(jnp.concatenate(parts, axis=1))
        mixed = dot(z, jnp.concatenate([dh, dl, dh], axis=0))
        for k in range(2):
            put(out, base + q + k, mixed[:, 128 * k : 128 * k + 128] + bases[k])


def analysis_kernel(pairs, outer, *refs):
    e0, e1, i0, i1, gram_in, pulled_in, wv0, wv1 = refs[:8]
    refs = refs[8:]
    step = pl.program_id(0)
    pair = (pairs[0] - 1) // 2 + step
    if outer:
        above, below, left_e, right_e, left_i, right_i = refs[:6]
        refs = refs[6:]
    out, h0, l0, h1, l1, g0, g1, sum0, sum1 = refs
    patches = [
        (e, n, (pair + i // 2) % 4, i % 2) for i, (e, n) in enumerate(((e0, i0),) * 2 + ((e1, i1),) * 2)
    ]
    works = ((0, wv0, h0, l0, g0, sum0), (1, wv1, h1, l1, g1, sum1))
    fars = [None, None]
    if outer:
        at_end = pair == 3

        @pl.when(at_end)
        def _():
            far_e = [(right_e, False, True), (left_e, True, True)]
            for k, wv, h, l, g, held in works:
                gram, total = gram_of(
                    ("edge", "halo"), 0, *patches[k : k + 3], above, below, far_e[k], wv, h, l, g
                )
                g[0] = gram
                held[...] = total

        @pl.when(jnp.logical_not(at_end))
        def _():
            for k, wv, h, l, g, held in works:
                g[0] = gram_in[k]
                held[...] = pulled_in[k]

        fars = [(right_i, False, at_end), (left_i, True, at_end)]
    for k, wv, h, l, g, held in works:
        early_gram = g.at[0] if outer else gram_in.at[k]
        early_total = held if outer else pulled_in.at[k]
        gram, total = gram_of(
            ("inner",), 16, *patches[k : k + 3], None, None, fars[k], wv, h, l, g.at[pl.ds(1, 2)]
        )
        analyse(gram + early_gram[...], total + early_total[...], patches[k + 1], out, 8 * k)


def analysis(edge, inner, grams, pulls, wv, pairs, *ends):
    outer = pairs[-1] == 7
    steps = len(pairs)
    start = (pairs[0] - 1) // 2

    def block(shift):
        return pl.BlockSpec((256, 8, 128), lambda i: (0, (start + i + shift) % 4, 0))

    def cells(shift):
        return pl.BlockSpec((1, 72, 128), lambda i: ((2 * (start + i) + 1 + shift) % 8, 0, 0))

    def held(width):
        return pl.BlockSpec((2, 256, width), lambda i: (jnp.minimum(start + i, 2), 0, 0))

    args = [edge, edge, inner, inner, grams, pulls, wv, wv]
    specs = [block(0), block(1), block(0), block(1), held(256), held(128), cells(0), cells(1)]
    if outer:
        args += list(ends)
        specs += [whole(v.shape) for v in ends]
    return pl.pallas_call(
        functools.partial(analysis_kernel, pairs, outer),
        grid=(steps,),
        in_specs=specs,
        out_specs=pl.BlockSpec((256, 16, 128), lambda i: (0, i, 0)),
        out_shape=jax.ShapeDtypeStruct((256, 16 * steps, 128), F32),
        scratch_shapes=[pltpu.VMEM((256, 2048), BF16)] * 4
        + [pltpu.VMEM((3, 256, 256), F32)] * 2
        + [pltpu.VMEM((256, 128), F32)] * 2,
        compiler_params=pltpu.CompilerParams(vmem_limit_bytes=60000 * 1024),
        cost_estimate=pl.CostEstimate(
            flops=steps * 12 * 10**9, bytes_accessed=steps * 6 * 2**20, transcendentals=0
        ),
        name="analysis",
    )(*args)


def shards(background, obs_cells, obs_counts, obs_widths, obs_values, obs_variances):
    axes = ("gx", "gy")
    gx, gy = lax.axis_size("gx"), lax.axis_size("gy")
    onward = [(i, i + 1) for i in range(gy - 1)]
    ring = [(i, (i + 1) % gx) for i in range(gx)]

    def exchange(x):
        return lax.all_to_all(x, axes, split_axis=0, concat_axis=0, tiled=True)

    def beside(pair):
        to_left, to_right = pair
        left = lax.ppermute(to_right, "gx", ring)
        return left, lax.ppermute(to_left, "gx", [(j, i) for i, j in ring])

    edge = exchange(pack(background, True).reshape(256, 32, 128))
    send = pack(background, False).reshape(256, 32, 128)
    wv = cell_sums(obs_cells[0], obs_counts[0], obs_widths[0], obs_values[0], obs_variances[0])
    tiles = edge.reshape(256, 4, 8, 128)
    up = tiles[:, :, 0:4].reshape(256, 16, 128)
    dn = tiles[:, :, 4:8].reshape(256, 16, 128)
    send, up, dn = lax.optimization_barrier((send, up, dn))
    above = lax.ppermute(dn, "gy", onward)
    below = lax.ppermute(up, "gy", [(j, i) for i, j in onward])
    inner = exchange(send)
    left_e, right_e = beside(sides(edge, ("edge", "halo"), above, below))
    grams, pulls = early(edge, above, below, wv)
    to_beside = sides(inner, ("inner",))
    left_i, right_i = beside(to_beside)
    ends = (above, below, left_e, right_e, left_i, right_i)
    results, order = [], []
    for pairs in (FIRST, SECOND):
        out = analysis(edge, inner, grams, pulls, wv, pairs, *ends)
        if pairs is FIRST:
            out, _ = lax.optimization_barrier((out, to_beside[0]))
        results.append(exchange(out))
        order.append([q % 8 for p in pairs for q in (p, p + 1)])
    a, b = [r.reshape(4, 32, 2, r.shape[1], 128) for r in results]
    return unpack(a, b, order)


def solution(mesh):
    return jax.shard_map(
        shards,
        mesh=mesh,
        in_specs=(
            P(("gx", "gy"), None, None, None),
            P("gy", "gx", None),
            P("gy", "gx"),
            P("gy", "gx"),
            P("gy", "gx", None),
            P("gy", "gx", None),
        ),
        out_specs=P(("gx", "gy"), None, None, None),
        check_vma=False,
    )
```

```python
import functools

import jax
import jax.numpy as jnp
from jax import lax
from jax.experimental import pallas as pl
from jax.experimental.pallas import tpu as pltpu
from jax.sharding import PartitionSpec as P

F32 = jnp.float32
BF16 = jnp.bfloat16
ITERS = 5
FIRST, SECOND = (1, 3), (5, 7)


def lane_group(shape):
    return lax.broadcasted_iota(jnp.int32, shape, len(shape) - 1) // 16


def skew(tiles):
    group = lane_group(tiles[0].shape)
    for bit in (1, 2, 4):
        odd = (group & bit) != 0
        tiles = [jnp.where(odd, tiles[(k + bit) % 8], tiles[k]) for k in range(8)]
    return tiles


def edge_lanes():
    shape = (8, 128)
    low = lax.broadcasted_iota(jnp.int32, shape, 0) < 4
    return (lane_group(shape) % 2 == 0) == low


def pack_kernel(x_ref, o_ref, *, edge):
    bands = o_ref.shape[1]
    first = edge_lanes()
    for band in range(bands):
        for member in range(2):
            for col in range(4):
                tiles = []
                for t in range(8):
                    row = 16 * band + 8 * (t % 2)
                    tile = x_ref[member, t // 2, row : row + 8, 128 * col : 128 * col + 128]
                    tiles.append(pltpu.roll(tile, 16 * t, 1) if t else tile)
                tiles = skew(tiles)
                for i in range(4):
                    even, odd = tiles[(8 - 2 * i) % 8], tiles[7 - 2 * i]
                    merged = jnp.where(first, even, odd) if edge else jnp.where(first, odd, even)
                    o_ref[col, band, member, 8 * i : 8 * i + 8, :] = merged


def pack(x, edge, bands=2):
    return pl.pallas_call(
        functools.partial(pack_kernel, edge=edge),
        grid=(32 // bands,),
        in_specs=[pl.BlockSpec((2, 4, 16 * bands, 512), lambda i: (0, 0, i, 0))],
        out_specs=pl.BlockSpec((4, bands, 2, 32, 128), lambda i: (0, i, 0, 0, 0)),
        out_shape=jax.ShapeDtypeStruct((4, 32, 2, 32, 128), F32),
        cost_estimate=pl.CostEstimate(flops=10**10, bytes_accessed=12 * 2**20, transcendentals=0),
        name="pack_edge" if edge else "pack_inner",
    )(x)


def unpack_kernel(a_ref, b_ref, o_ref, *, order):
    bands = a_ref.shape[1]
    place = {p: (a_ref, i) for i, p in enumerate(order[0])}
    place.update({p: (b_ref, i) for i, p in enumerate(order[1])})
    for band in range(bands):
        for member in range(2):
            for col in range(4):
                tiles = []
                for p in range(8):
                    ref, i = place[p]
                    tiles.append(ref[col, band, member, 8 * i : 8 * i + 8, :])
                tiles = skew(tiles)
                for t in range(8):
                    tile = tiles[(8 - t) % 8]
                    tile = pltpu.roll(tile, 128 - 16 * t, 1) if t else tile
                    row = 16 * band + 8 * (t % 2)
                    o_ref[member, t // 2, row : row + 8, 128 * col : 128 * col + 128] = tile


def unpack(a, b, order, bands=2):
    na, nb = 8 * len(order[0]), 8 * len(order[1])
    return pl.pallas_call(
        functools.partial(unpack_kernel, order=order),
        grid=(32 // bands,),
        in_specs=[
            pl.BlockSpec((4, bands, 2, na, 128), lambda i: (0, i, 0, 0, 0)),
            pl.BlockSpec((4, bands, 2, nb, 128), lambda i: (0, i, 0, 0, 0)),
        ],
        out_specs=pl.BlockSpec((2, 4, 16 * bands, 512), lambda i: (0, 0, i, 0)),
        out_shape=jax.ShapeDtypeStruct((2, 4, 512, 512), F32),
        name="unpack",
    )(a, b)


def three_way(x):
    high = x.astype(BF16)
    rest = x - high.astype(F32)
    mid = rest.astype(BF16)
    return high, mid, (rest - mid.astype(F32)).astype(BF16)


def two_way(x):
    high = x.astype(BF16)
    return high, (x - high.astype(F32)).astype(BF16)


def cells_kernel(kc_ref, lane_ref, w_ref, v_ref, o_ref):
    kc = kc_ref[0]
    slots = kc.shape[1]
    row_hit = lax.broadcasted_iota(jnp.int32, (24, slots), 0) == kc
    lane_hit = lax.broadcasted_iota(jnp.int32, (128, slots), 0) == lane_ref[0]
    lane_hot = jnp.where(lane_hit, 1.0, 0.0).astype(BF16)
    both = jnp.concatenate(
        [jnp.where(row_hit, w_ref[0], 0.0), jnp.where(row_hit, v_ref[0], 0.0)], axis=0
    )
    total = jnp.zeros((48, 128), F32)
    for part in three_way(both):
        total = total + lax.dot_general(
            part, lane_hot, (((1,), (1,)), ((), ())), preferred_element_type=F32
        )
    w = total[:24]
    root = jnp.where(w > 0.0, jnp.sqrt(jnp.maximum(w, 1e-30)), 0.0)
    o_ref[0] = jnp.concatenate([total, root], axis=0)


def cell_sums(obs_cells, obs_counts, obs_widths, obs_values, obs_variances):
    number, slots = obs_cells.shape
    level = obs_cells // 576
    row = obs_cells // 24 % 24
    col = obs_cells % 24
    row_out = jnp.maximum(jnp.maximum(4 - row, row - 19), 0)
    col_out = jnp.maximum(jnp.maximum(4 - col, col - 19), 0)
    distance = jnp.maximum(row_out, col_out)
    slot = lax.broadcasted_iota(jnp.int32, obs_cells.shape, 1)
    usable = (slot < obs_counts[:, None]) & (distance <= obs_widths[:, None])
    relative = distance.astype(F32) / (obs_widths[:, None] + 1).astype(F32)
    w = jnp.where(usable, jnp.exp(-relative * relative) / obs_variances, 0.0)
    v = w * obs_values
    t = 2 * level + jnp.where((row >= 12) & (row < 20) | (row < 4), 1, 0)
    halo = (row < 4) | (row >= 20)
    inside = (row >= 8) & (row < 16)
    west, east = col < 4, col >= 20
    shift = jnp.where(west, -1, jnp.where(east, 1, 0))
    inner = jnp.where(west, 12 + col, jnp.where(east, col - 20, col - 4))
    p = lax.broadcasted_iota(jnp.int32, obs_cells.shape, 0)
    lane = 16 * ((t + p + shift + 8) % 8) + inner
    side = jnp.where(west | east, 1, 0)
    kc = row % 4 + jnp.where(inside, 16 + 4 * side, 8 * side + jnp.where(halo, 4, 0))
    spec = pl.BlockSpec((1, 1, slots), lambda i: (i, 0, 0))
    shape = (number, 1, slots)
    return pl.pallas_call(
        cells_kernel,
        grid=(number,),
        in_specs=[spec] * 4,
        out_specs=pl.BlockSpec((1, 72, 128), lambda i: (i, 0, 0)),
        out_shape=jax.ShapeDtypeStruct((number, 72, 128), F32),
        cost_estimate=pl.CostEstimate(flops=5 * 10**9, bytes_accessed=2**20, transcendentals=0),
        name="cells",
    )(kc.reshape(shape), lane.reshape(shape), w.reshape(shape), v.reshape(shape))


def take(ref, row):
    members, rows, lanes = ref.shape
    return ref.reshape(members * rows, lanes)[pl.ds(row, members, stride=rows), :]


def put(ref, row, value):
    members, rows, lanes = ref.shape
    ref.reshape(members * rows, lanes)[pl.ds(row, members, stride=rows), :] = value


def odd_rows(odd):
    return ((lane_group((1, 128)) - odd) & 1) == 1


def column(kind, q, patch, above, below):
    edge, inner, pair, odd = patch
    if kind == "edge":
        a, b = take(edge, q), take(edge, 4 + q)
    elif kind == "inner":
        a, b = take(inner, 4 + q), take(inner, q)
    else:
        a, b = take(below, 4 * pair + q), take(above, 4 * pair + q)
    return jnp.where(odd_rows(odd), b, a)


def sides_kernel(*refs, kinds):
    count = len(kinds)
    first_ref, last_ref = refs[:2]
    above, below = refs[2:4] if "halo" in kinds else (None, None)
    left_ref, right_ref = refs[-2:]
    within = lax.broadcasted_iota(jnp.int32, (1, 128), 1) % 16 // 4
    for j in range(count):
        left = right = None
        for i in range(4):
            f = column(kinds[j], i, (first_ref, first_ref, 0, 0), above, below)
            f = pltpu.roll(f, 4 * i, 1) if i else f
            l = column(kinds[j], i, (last_ref, last_ref, 3, 1), above, below)
            l = pltpu.roll(l, 128 - 4 * (3 - i), 1) if i < 3 else l
            left = f if left is None else jnp.where(within == i, f, left)
            right = l if right is None else jnp.where(within == i, l, right)
        left_ref[:, 128 * j : 128 * j + 128] = left
        right_ref[:, 128 * j : 128 * j + 128] = right


def whole(shape):
    return pl.BlockSpec(shape, lambda i: (0,) * len(shape))


def sides(x, kinds, *halo):
    width = 128 * len(kinds)
    return pl.pallas_call(
        functools.partial(sides_kernel, kinds=kinds),
        grid=(1,),
        in_specs=[
            pl.BlockSpec((256, 8, 128), lambda i: (0, 0, 0)),
            pl.BlockSpec((256, 8, 128), lambda i: (0, 3, 0)),
        ]
        + [whole((256, 16, 128))] * len(halo),
        out_specs=[whole((256, width))] * 2,
        out_shape=[jax.ShapeDtypeStruct((256, width), F32)] * 2,
        cost_estimate=pl.CostEstimate(flops=10**9, bytes_accessed=4 * 2**20, transcendentals=0),
        name="sides",
    )(x, x, *halo)


def dot(a, b):
    return jnp.dot(a, b, preferred_element_type=F32)


def product(a, b):
    (ah, al), (bh, bl) = a, b
    return dot(jnp.concatenate([ah, ah, al], axis=1), jnp.concatenate([bh, bl, bh], axis=0))


def gram_of(kinds, base, west, mine, east, above, below, far, wv, high_ref, low_ref, gram_ref):
    total = jnp.zeros((256, 128), F32)
    within = lax.broadcasted_iota(jnp.int32, (1, 128), 1) % 16
    place = 0
    for strip in (False, True):
        for j, kind in enumerate(kinds):
            for q in range(4):
                if not strip:
                    x = column(kind, q, mine, above, below)
                else:
                    l = column(kind, q, west, above, below)
                    r = column(kind, q, east, above, below)
                    if far is not None:
                        ref, from_west, outer = far
                        v = ref[:, 128 * j : 128 * j + 128]
                        if from_west:
                            v = pltpu.roll(v, 4 * (3 - q), 1) if q < 3 else v
                            l = jnp.where(outer, v, l)
                        else:
                            v = pltpu.roll(v, 128 - 4 * q, 1) if q else v
                            r = jnp.where(outer, v, r)
                    x = jnp.where(within < 8, r, l)
                c = base + place
                w = wv[0, c : c + 1, :]
                v = wv[0, 24 + c : 25 + c, :]
                root = wv[0, 48 + c : 49 + c, :]
                mean = jnp.sum(x, axis=0, keepdims=True) * (1.0 / 256)
                dev = x - mean
                total = total + dev * (v - w * mean)
                high, low = two_way(dev * root)
                high_ref[:, 128 * place : 128 * place + 128] = high
                low_ref[:, 128 * place : 128 * place + 128] = low
                place += 1
    nt = (((1,), (1,)), ((), ()))
    high, low = high_ref[:, : 128 * place], low_ref[:, : 128 * place]
    gram_ref[0] = lax.dot_general(high, high, nt, preferred_element_type=F32)
    gram_ref[1] = lax.dot_general(high, low, nt, preferred_element_type=F32)
    cross = gram_ref[1]
    return gram_ref[0] + (cross + cross.T), total


def early_kernel(
    e0, e1, above, below, left, right, wv0, wv1, gram_out, pulled_out, h0, l0, h1, l1, g0, g1
):
    pair = pl.program_id(0)
    patches = [(e, None, (pair + i // 2) % 4, i % 2) for i, e in enumerate((e0, e0, e1, e1))]
    fars = ((right, False, pair == 3), (left, True, pair == 3))
    for k, wv, h, l, g in ((0, wv0, h0, l0, g0), (1, wv1, h1, l1, g1)):
        gram, total = gram_of(
            ("edge", "halo"), 0, *patches[k : k + 3], above, below, fars[k], wv, h, l, g
        )
        gram_out[k] = gram
        pulled_out[k] = total


def early(edge, above, below, left, right, wv):
    steps = 4
    return pl.pallas_call(
        early_kernel,
        grid=(steps,),
        in_specs=[
            pl.BlockSpec((256, 8, 128), lambda i: (0, i, 0)),
            pl.BlockSpec((256, 8, 128), lambda i: (0, (i + 1) % 4, 0)),
            whole((256, 16, 128)),
            whole((256, 16, 128)),
            whole((256, 256)),
            whole((256, 256)),
            pl.BlockSpec((1, 72, 128), lambda i: (2 * i + 1, 0, 0)),
            pl.BlockSpec((1, 72, 128), lambda i: ((2 * i + 2) % 8, 0, 0)),
        ],
        out_specs=[
            pl.BlockSpec((2, 256, 256), lambda i: (i, 0, 0)),
            pl.BlockSpec((2, 256, 128), lambda i: (i, 0, 0)),
        ],
        out_shape=[
            jax.ShapeDtypeStruct((8, 256, 256), F32),
            jax.ShapeDtypeStruct((8, 256, 128), F32),
        ],
        scratch_shapes=[pltpu.VMEM((256, 2048), BF16)] * 4 + [pltpu.VMEM((2, 256, 256), F32)] * 2,
        compiler_params=pltpu.CompilerParams(vmem_limit_bytes=60000 * 1024),
        cost_estimate=pl.CostEstimate(
            flops=20 * 10**9, bytes_accessed=12 * 2**20, transcendentals=0
        ),
        name="early",
    )(edge, edge, above, below, left, right, wv, wv)


def newton(s0, s1, last):
    row = lax.broadcasted_iota(jnp.int32, (256, 256), 0)
    col = lax.broadcasted_iota(jnp.int32, (256, 256), 1)
    eye = jnp.where(row == col, 1.5, 0.0)
    halves = [(two_way(s[0]), two_way(s[1])) for s in (s0, s1)]
    both = [product(inv, cur) for cur, inv in halves]
    factors = [two_way(eye - 0.5 * x) for x in both]
    if not last:
        for s, (cur, _), factor in zip((s0, s1), halves, factors):
            s[0] = product(cur, factor)
    for s, (_, inv), factor in zip((s0, s1), halves, factors):
        s[1] = product(factor, inv)


def start_newton(gram, s):
    squares = jnp.sum(jnp.sum(gram * gram, axis=0, keepdims=True), axis=1, keepdims=True)
    divisor = 255.0 + jnp.sqrt(jnp.maximum(squares, 1e-30))
    row = lax.broadcasted_iota(jnp.int32, (256, 256), 0)
    col = lax.broadcasted_iota(jnp.int32, (256, 256), 1)
    eye = row == col
    current = (gram + jnp.where(eye, 255.0, 0.0)) / divisor
    inverse = jnp.where(eye, 1.5, 0.0) - 0.5 * current
    s[0] = product(two_way(current), two_way(inverse))
    s[1] = inverse
    return divisor


def apply(inverse, pulled, divisor, mine, out, base):
    halfway = jnp.sum(inverse * pulled, axis=0, keepdims=True)
    weight = jnp.sum(inverse * halfway, axis=1, keepdims=True) / divisor
    zh, zl = two_way(inverse * jnp.sqrt(255.0 / divisor))
    z = jnp.concatenate([zh, zh, zl], axis=1)
    edge, inner, _, odd = mine
    for q in range(0, 8, 2):
        parts, bases = [], []
        for k in range(2):
            a, b = take(edge, q + k), take(inner, q + k)
            x = jnp.where(odd_rows(odd), b, a) if q < 4 else jnp.where(odd_rows(odd), a, b)
            centre = jnp.sum(x, axis=0, keepdims=True) * (1.0 / 256)
            dev = x - centre
            bases.append(centre + jnp.sum(dev * weight, axis=0, keepdims=True))
            parts.append(dev)
        dh, dl = two_way(jnp.concatenate(parts, axis=1))
        mixed = dot(z, jnp.concatenate([dh, dl, dh], axis=0))
        for k in range(2):
            put(out, base + q + k, mixed[:, 128 * k : 128 * k + 128] + bases[k])


def analysis_kernel(pairs, outer, *refs):
    e0, e1, i0, i1, gram_in, pulled_in, wv0, wv1 = refs[:8]
    refs = refs[8:]
    step = pl.program_id(0)
    pair = (pairs[0] - 1) // 2 + step
    fars = [None, None]
    if outer:
        fars = [(refs[1], False, pair == 3), (refs[0], True, pair == 3)]
        refs = refs[2:]
    out, h0, l0, h1, l1, g0, g1, s0, s1 = refs
    patches = [
        (e, n, (pair + i // 2) % 4, i % 2) for i, (e, n) in enumerate(((e0, i0),) * 2 + ((e1, i1),) * 2)
    ]
    pulled, divisors = [], []
    for k, wv, h, l, g, s in ((0, wv0, h0, l0, g0, s0), (1, wv1, h1, l1, g1, s1)):
        gram, total = gram_of(("inner",), 16, *patches[k : k + 3], None, None, fars[k], wv, h, l, g)
        pulled.append(jnp.sum(total + pulled_in[k], axis=1, keepdims=True))
        divisors.append(start_newton(gram + gram_in[k], s))

    def body(_, carry):
        newton(s0, s1, False)
        return carry

    lax.fori_loop(0, ITERS - 2, body, 0)
    newton(s0, s1, True)
    for k, s in ((0, s0), (1, s1)):
        apply(s[1], pulled[k], divisors[k], patches[k + 1], out, 8 * k)


def analysis(edge, inner, grams, pulls, wv, pairs, *ends):
    outer = pairs[-1] == 7
    steps = len(pairs)
    start = (pairs[0] - 1) // 2

    def block(shift):
        return pl.BlockSpec((256, 8, 128), lambda i: (0, (start + i + shift) % 4, 0))

    def cells(shift):
        return pl.BlockSpec((1, 72, 128), lambda i: ((2 * (start + i) + 1 + shift) % 8, 0, 0))

    def held(width):
        return pl.BlockSpec((2, 256, width), lambda i: (start + i, 0, 0))

    args = [edge, edge, inner, inner, grams, pulls, wv, wv]
    specs = [block(0), block(1), block(0), block(1), held(256), held(128), cells(0), cells(1)]
    if outer:
        args += list(ends)
        specs += [whole(v.shape) for v in ends]
    return pl.pallas_call(
        functools.partial(analysis_kernel, pairs, outer),
        grid=(steps,),
        in_specs=specs,
        out_specs=pl.BlockSpec((256, 16, 128), lambda i: (0, i, 0)),
        out_shape=jax.ShapeDtypeStruct((256, 16 * steps, 128), F32),
        scratch_shapes=[pltpu.VMEM((256, 1024), BF16)] * 4 + [pltpu.VMEM((2, 256, 256), F32)] * 4,
        compiler_params=pltpu.CompilerParams(vmem_limit_bytes=60000 * 1024),
        cost_estimate=pl.CostEstimate(
            flops=steps * 12 * 10**9, bytes_accessed=steps * 6 * 2**20, transcendentals=0
        ),
        name="analysis",
    )(*args)


def shards(background, obs_cells, obs_counts, obs_widths, obs_values, obs_variances):
    axes = ("gx", "gy")
    gx, gy = lax.axis_size("gx"), lax.axis_size("gy")
    onward = [(i, i + 1) for i in range(gy - 1)]
    ring = [(i, (i + 1) % gx) for i in range(gx)]

    def exchange(x):
        return lax.all_to_all(x, axes, split_axis=0, concat_axis=0, tiled=True)

    def beside(pair):
        to_left, to_right = pair
        left = lax.ppermute(to_right, "gx", ring)
        return left, lax.ppermute(to_left, "gx", [(j, i) for i, j in ring])

    edge = exchange(pack(background, True).reshape(256, 32, 128))
    send = pack(background, False).reshape(256, 32, 128)
    wv = cell_sums(obs_cells[0], obs_counts[0], obs_widths[0], obs_values[0], obs_variances[0])
    tiles = edge.reshape(256, 4, 8, 128)
    up = tiles[:, :, 0:4].reshape(256, 16, 128)
    dn = tiles[:, :, 4:8].reshape(256, 16, 128)
    above = lax.ppermute(dn, "gy", onward)
    below = lax.ppermute(up, "gy", [(j, i) for i, j in onward])
    left_e, right_e = beside(sides(edge, ("edge", "halo"), above, below))
    send, wv, left_e, right_e = lax.optimization_barrier((send, wv, left_e, right_e))
    inner = exchange(send)
    grams, pulls = early(edge, above, below, left_e, right_e, wv)
    left_i, right_i = beside(sides(inner, ("inner",)))
    ends = (left_i, right_i)
    results, order = [], []
    for pairs in (FIRST, SECOND):
        out = analysis(edge, inner, grams, pulls, wv, pairs, *ends)
        if pairs is FIRST:
            out, *ends = lax.optimization_barrier((out, *ends))
        results.append(exchange(out))
        order.append([q % 8 for p in pairs for q in (p, p + 1)])
    a, b = [r.reshape(4, 32, 2, r.shape[1], 128) for r in results]
    return unpack(a, b, order)


def solution(mesh):
    return jax.shard_map(
        shards,
        mesh=mesh,
        in_specs=(
            P(("gx", "gy"), None, None, None),
            P("gy", "gx", None),
            P("gy", "gx"),
            P("gy", "gx"),
            P("gy", "gx", None),
            P("gy", "gx", None),
        ),
        out_specs=P(("gx", "gy"), None, None, None),
        check_vma=False,
    )
```

```python
import functools

import jax
import jax.numpy as jnp
from jax import lax
from jax.experimental import pallas as pl
from jax.experimental.pallas import tpu as pltpu
from jax.sharding import PartitionSpec as P

F32 = jnp.float32
BF16 = jnp.bfloat16
ITERS = 5
FIRST, SECOND = (1, 3), (5, 7)


def lane_group(shape):
    return lax.broadcasted_iota(jnp.int32, shape, len(shape) - 1) // 16


def skew(tiles):
    group = lane_group(tiles[0].shape)
    for bit in (1, 2, 4):
        odd = (group & bit) != 0
        tiles = [jnp.where(odd, tiles[(k + bit) % 8], tiles[k]) for k in range(8)]
    return tiles


def edge_lanes():
    shape = (8, 128)
    low = lax.broadcasted_iota(jnp.int32, shape, 0) < 4
    return (lane_group(shape) % 2 == 0) == low


def pack_kernel(x_ref, o_ref, *, edge):
    first = edge_lanes()

    @pl.loop(0, o_ref.shape[1])
    def _(band):
        for member in range(2):
            for col in range(4):
                tiles = []
                for t in range(8):
                    rows = pl.ds(pl.multiple_of(16 * band + 8 * (t % 2), 8), 8)
                    tile = x_ref[member, t // 2, rows, 128 * col : 128 * col + 128]
                    tiles.append(pltpu.roll(tile, 16 * t, 1) if t else tile)
                tiles = skew(tiles)
                for i in range(4):
                    even, odd = tiles[(8 - 2 * i) % 8], tiles[7 - 2 * i]
                    merged = jnp.where(first, even, odd) if edge else jnp.where(first, odd, even)
                    o_ref[col, band, member, 8 * i : 8 * i + 8, :] = merged


def pack(x, edge, bands=8):
    return pl.pallas_call(
        functools.partial(pack_kernel, edge=edge),
        grid=(32 // bands,),
        in_specs=[pl.BlockSpec((2, 4, 16 * bands, 512), lambda i: (0, 0, i, 0))],
        out_specs=pl.BlockSpec((4, bands, 2, 32, 128), lambda i: (0, i, 0, 0, 0)),
        out_shape=jax.ShapeDtypeStruct((4, 32, 2, 32, 128), F32),
        cost_estimate=pl.CostEstimate(flops=10**10, bytes_accessed=12 * 2**20, transcendentals=0),
        name="pack_edge" if edge else "pack_inner",
    )(x)


def unpack_kernel(a_ref, b_ref, o_ref, *, order):
    place = {p: (a_ref, i) for i, p in enumerate(order[0])}
    place.update({p: (b_ref, i) for i, p in enumerate(order[1])})

    @pl.loop(0, a_ref.shape[1])
    def _(band):
        for member in range(2):
            for col in range(4):
                tiles = []
                for p in range(8):
                    ref, i = place[p]
                    tiles.append(ref[col, band, member, 8 * i : 8 * i + 8, :])
                tiles = skew(tiles)
                for t in range(8):
                    tile = tiles[(8 - t) % 8]
                    tile = pltpu.roll(tile, 128 - 16 * t, 1) if t else tile
                    rows = pl.ds(pl.multiple_of(16 * band + 8 * (t % 2), 8), 8)
                    o_ref[member, t // 2, rows, 128 * col : 128 * col + 128] = tile


def unpack(a, b, order, bands=8):
    na, nb = 8 * len(order[0]), 8 * len(order[1])
    return pl.pallas_call(
        functools.partial(unpack_kernel, order=order),
        grid=(32 // bands,),
        in_specs=[
            pl.BlockSpec((4, bands, 2, na, 128), lambda i: (0, i, 0, 0, 0)),
            pl.BlockSpec((4, bands, 2, nb, 128), lambda i: (0, i, 0, 0, 0)),
        ],
        out_specs=pl.BlockSpec((2, 4, 16 * bands, 512), lambda i: (0, 0, i, 0)),
        out_shape=jax.ShapeDtypeStruct((2, 4, 512, 512), F32),
        name="unpack",
    )(a, b)


def three_way(x):
    high = x.astype(BF16)
    rest = x - high.astype(F32)
    mid = rest.astype(BF16)
    return high, mid, (rest - mid.astype(F32)).astype(BF16)


def two_way(x):
    high = x.astype(BF16)
    return high, (x - high.astype(F32)).astype(BF16)


def cells_kernel(kc_ref, lane_ref, w_ref, v_ref, o_ref):
    kc = kc_ref[0]
    slots = kc.shape[1]
    row_hit = lax.broadcasted_iota(jnp.int32, (24, slots), 0) == kc
    lane_hit = lax.broadcasted_iota(jnp.int32, (128, slots), 0) == lane_ref[0]
    lane_hot = jnp.where(lane_hit, 1.0, 0.0).astype(BF16)
    both = jnp.concatenate(
        [jnp.where(row_hit, w_ref[0], 0.0), jnp.where(row_hit, v_ref[0], 0.0)], axis=0
    )
    total = jnp.zeros((48, 128), F32)
    for part in three_way(both):
        total = total + lax.dot_general(
            part, lane_hot, (((1,), (1,)), ((), ())), preferred_element_type=F32
        )
    w = total[:24]
    root = jnp.where(w > 0.0, jnp.sqrt(jnp.maximum(w, 1e-30)), 0.0)
    o_ref[0] = jnp.concatenate([total, root], axis=0)


def cell_sums(obs_cells, obs_counts, obs_widths, obs_values, obs_variances):
    number, slots = obs_cells.shape
    level = obs_cells // 576
    row = obs_cells // 24 % 24
    col = obs_cells % 24
    row_out = jnp.maximum(jnp.maximum(4 - row, row - 19), 0)
    col_out = jnp.maximum(jnp.maximum(4 - col, col - 19), 0)
    distance = jnp.maximum(row_out, col_out)
    slot = lax.broadcasted_iota(jnp.int32, obs_cells.shape, 1)
    usable = (slot < obs_counts[:, None]) & (distance <= obs_widths[:, None])
    relative = distance.astype(F32) / (obs_widths[:, None] + 1).astype(F32)
    w = jnp.where(usable, jnp.exp(-relative * relative) / obs_variances, 0.0)
    v = w * obs_values
    t = 2 * level + jnp.where((row >= 12) & (row < 20) | (row < 4), 1, 0)
    halo = (row < 4) | (row >= 20)
    inside = (row >= 8) & (row < 16)
    west, east = col < 4, col >= 20
    shift = jnp.where(west, -1, jnp.where(east, 1, 0))
    inner = jnp.where(west, 12 + col, jnp.where(east, col - 20, col - 4))
    p = lax.broadcasted_iota(jnp.int32, obs_cells.shape, 0)
    lane = 16 * ((t + p + shift + 8) % 8) + inner
    side = jnp.where(west | east, 1, 0)
    kc = row % 4 + jnp.where(inside, 16 + 4 * side, 8 * side + jnp.where(halo, 4, 0))
    spec = pl.BlockSpec((1, 1, slots), lambda i: (i, 0, 0))
    shape = (number, 1, slots)
    return pl.pallas_call(
        cells_kernel,
        grid=(number,),
        in_specs=[spec] * 4,
        out_specs=pl.BlockSpec((1, 72, 128), lambda i: (i, 0, 0)),
        out_shape=jax.ShapeDtypeStruct((number, 72, 128), F32),
        cost_estimate=pl.CostEstimate(flops=5 * 10**9, bytes_accessed=2**20, transcendentals=0),
        name="cells",
    )(kc.reshape(shape), lane.reshape(shape), w.reshape(shape), v.reshape(shape))


def take(ref, row):
    members, rows, lanes = ref.shape
    return ref.reshape(members * rows, lanes)[pl.ds(row, members, stride=rows), :]


def put(ref, row, value):
    members, rows, lanes = ref.shape
    ref.reshape(members * rows, lanes)[pl.ds(row, members, stride=rows), :] = value


def odd_rows(odd):
    return ((lane_group((1, 128)) - odd) & 1) == 1


def column(kind, q, patch, above, below):
    edge, inner, pair, odd = patch
    if kind == "edge":
        a, b = take(edge, q), take(edge, 4 + q)
    elif kind == "inner":
        a, b = take(inner, 4 + q), take(inner, q)
    else:
        a, b = take(below, 4 * pair + q), take(above, 4 * pair + q)
    return jnp.where(odd_rows(odd), b, a)


def sides_kernel(*refs, kinds):
    count = len(kinds)
    first_ref, last_ref = refs[:2]
    above, below = refs[2:4] if "halo" in kinds else (None, None)
    left_ref, right_ref = refs[-2:]
    within = lax.broadcasted_iota(jnp.int32, (1, 128), 1) % 16 // 4
    for j in range(count):
        left = right = None
        for i in range(4):
            f = column(kinds[j], i, (first_ref, first_ref, 0, 0), above, below)
            f = pltpu.roll(f, 4 * i, 1) if i else f
            l = column(kinds[j], i, (last_ref, last_ref, 3, 1), above, below)
            l = pltpu.roll(l, 128 - 4 * (3 - i), 1) if i < 3 else l
            left = f if left is None else jnp.where(within == i, f, left)
            right = l if right is None else jnp.where(within == i, l, right)
        left_ref[:, 128 * j : 128 * j + 128] = left
        right_ref[:, 128 * j : 128 * j + 128] = right


def whole(shape):
    return pl.BlockSpec(shape, lambda i: (0,) * len(shape))


def sides(x, kinds, *halo):
    width = 128 * len(kinds)
    return pl.pallas_call(
        functools.partial(sides_kernel, kinds=kinds),
        grid=(1,),
        in_specs=[
            pl.BlockSpec((256, 8, 128), lambda i: (0, 0, 0)),
            pl.BlockSpec((256, 8, 128), lambda i: (0, 3, 0)),
        ]
        + [whole((256, 16, 128))] * len(halo),
        out_specs=[whole((256, width))] * 2,
        out_shape=[jax.ShapeDtypeStruct((256, width), F32)] * 2,
        cost_estimate=pl.CostEstimate(flops=10**9, bytes_accessed=4 * 2**20, transcendentals=0),
        name="sides",
    )(x, x, *halo)


def dot(a, b):
    return jnp.dot(a, b, preferred_element_type=F32)


def product(a, b):
    (ah, al), (bh, bl) = a, b
    return dot(jnp.concatenate([ah, ah, al], axis=1), jnp.concatenate([bh, bl, bh], axis=0))


def gram_of(kinds, base, west, mine, east, above, below, far, wv, high_ref, low_ref, gram_ref):
    total = jnp.zeros((256, 128), F32)
    within = lax.broadcasted_iota(jnp.int32, (1, 128), 1) % 16
    place = 0
    for strip in (False, True):
        for j, kind in enumerate(kinds):
            for q in range(4):
                if not strip:
                    x = column(kind, q, mine, above, below)
                else:
                    l = column(kind, q, west, above, below)
                    r = column(kind, q, east, above, below)
                    if far is not None:
                        ref, from_west, outer = far
                        v = ref[:, 128 * j : 128 * j + 128]
                        if from_west:
                            v = pltpu.roll(v, 4 * (3 - q), 1) if q < 3 else v
                            l = jnp.where(outer, v, l)
                        else:
                            v = pltpu.roll(v, 128 - 4 * q, 1) if q else v
                            r = jnp.where(outer, v, r)
                    x = jnp.where(within < 8, r, l)
                c = base + place
                w = wv[0, c : c + 1, :]
                v = wv[0, 24 + c : 25 + c, :]
                root = wv[0, 48 + c : 49 + c, :]
                mean = jnp.sum(x, axis=0, keepdims=True) * (1.0 / 256)
                dev = x - mean
                total = total + dev * (v - w * mean)
                high, low = two_way(dev * root)
                high_ref[:, 128 * place : 128 * place + 128] = high
                low_ref[:, 128 * place : 128 * place + 128] = low
                place += 1
    nt = (((1,), (1,)), ((), ()))
    high, low = high_ref[:, : 128 * place], low_ref[:, : 128 * place]
    gram_ref[0] = lax.dot_general(high, high, nt, preferred_element_type=F32)
    gram_ref[1] = lax.dot_general(high, low, nt, preferred_element_type=F32)
    cross = gram_ref[1]
    return gram_ref[0] + (cross + cross.T), total


def early_kernel(start, *refs):
    e0, e1, above, below, wv0, wv1 = refs[:6]
    gram_out, pulled_out, h0, l0, h1, l1, g0, g1 = refs[-8:]
    pair = start + pl.program_id(0)
    patches = [(e, None, (pair + i // 2) % 4, i % 2) for i, e in enumerate((e0, e0, e1, e1))]
    fars = [(refs[7], False, True), (refs[6], True, True)] if start == 3 else [None, None]
    for k, wv, h, l, g in ((0, wv0, h0, l0, g0), (1, wv1, h1, l1, g1)):
        gram, total = gram_of(
            ("edge", "halo"), 0, *patches[k : k + 3], above, below, fars[k], wv, h, l, g
        )
        gram_out[k] = gram
        pulled_out[k] = total


def early(edge, above, below, wv, start, steps, *last):
    args = [edge, edge, above, below, wv, wv, *last]
    specs = [
        pl.BlockSpec((256, 8, 128), lambda i: (0, start + i, 0)),
        pl.BlockSpec((256, 8, 128), lambda i: (0, (start + i + 1) % 4, 0)),
        whole((256, 16, 128)),
        whole((256, 16, 128)),
        pl.BlockSpec((1, 72, 128), lambda i: (2 * (start + i) + 1, 0, 0)),
        pl.BlockSpec((1, 72, 128), lambda i: ((2 * (start + i) + 2) % 8, 0, 0)),
    ]
    if last:
        specs += [whole((256, 256))] * 2 + [pl.BlockSpec(memory_space=pl.ANY)] * 2
    return pl.pallas_call(
        functools.partial(early_kernel, start),
        grid=(steps,),
        in_specs=specs,
        out_specs=[
            pl.BlockSpec((2, 256, 256), lambda i: (start + i, 0, 0)),
            pl.BlockSpec((2, 256, 128), lambda i: (start + i, 0, 0)),
        ],
        out_shape=[
            jax.ShapeDtypeStruct((8, 256, 256), F32),
            jax.ShapeDtypeStruct((8, 256, 128), F32),
        ],
        input_output_aliases={8: 0, 9: 1} if last else {},
        scratch_shapes=[pltpu.VMEM((256, 2048), BF16)] * 4 + [pltpu.VMEM((2, 256, 256), F32)] * 2,
        compiler_params=pltpu.CompilerParams(vmem_limit_bytes=58 * 1024 * 1024),
        cost_estimate=pl.CostEstimate(
            flops=steps * 7 * 10**9, bytes_accessed=steps * 4 * 2**20, transcendentals=0
        ),
        name="early",
    )(*args)


def newton(s0, s1, last):
    row = lax.broadcasted_iota(jnp.int32, (256, 256), 0)
    col = lax.broadcasted_iota(jnp.int32, (256, 256), 1)
    eye = jnp.where(row == col, 1.5, 0.0)
    halves = [(two_way(s[0]), two_way(s[1])) for s in (s0, s1)]
    both = [product(inv, cur) for cur, inv in halves]
    factors = [two_way(eye - 0.5 * x) for x in both]
    if not last:
        for s, (cur, _), factor in zip((s0, s1), halves, factors):
            s[0] = product(cur, factor)
    for s, (_, inv), factor in zip((s0, s1), halves, factors):
        s[1] = product(factor, inv)


def start_newton(gram, s):
    squares = jnp.sum(jnp.sum(gram * gram, axis=0, keepdims=True), axis=1, keepdims=True)
    divisor = 255.0 + jnp.sqrt(jnp.maximum(squares, 1e-30))
    row = lax.broadcasted_iota(jnp.int32, (256, 256), 0)
    col = lax.broadcasted_iota(jnp.int32, (256, 256), 1)
    eye = row == col
    current = (gram + jnp.where(eye, 255.0, 0.0)) / divisor
    inverse = jnp.where(eye, 1.5, 0.0) - 0.5 * current
    s[0] = product(two_way(current), two_way(inverse))
    s[1] = inverse
    return divisor


def apply(inverse, pulled, divisor, mine, out, base):
    halfway = jnp.sum(inverse * pulled, axis=0, keepdims=True)
    weight = jnp.sum(inverse * halfway, axis=1, keepdims=True) / divisor
    zh, zl = two_way(inverse * jnp.sqrt(255.0 / divisor))
    z = jnp.concatenate([zh, zh, zl], axis=1)
    edge, inner, _, odd = mine
    for q in range(0, 8, 2):
        parts, bases = [], []
        for k in range(2):
            a, b = take(edge, q + k), take(inner, q + k)
            x = jnp.where(odd_rows(odd), b, a) if q < 4 else jnp.where(odd_rows(odd), a, b)
            centre = jnp.sum(x, axis=0, keepdims=True) * (1.0 / 256)
            dev = x - centre
            bases.append(centre + jnp.sum(dev * weight, axis=0, keepdims=True))
            parts.append(dev)
        dh, dl = two_way(jnp.concatenate(parts, axis=1))
        mixed = dot(z, jnp.concatenate([dh, dl, dh], axis=0))
        for k in range(2):
            put(out, base + q + k, mixed[:, 128 * k : 128 * k + 128] + bases[k])


def analysis_kernel(pairs, outer, *refs):
    e0, e1, i0, i1, gram_in, pulled_in, wv0, wv1 = refs[:8]
    refs = refs[8:]
    step = pl.program_id(0)
    pair = (pairs[0] - 1) // 2 + step
    fars = [None, None]
    if outer:
        fars = [(refs[1], False, pair == 3), (refs[0], True, pair == 3)]
        refs = refs[2:]
    out, h0, l0, h1, l1, g0, g1, s0, s1 = refs
    patches = [
        (e, n, (pair + i // 2) % 4, i % 2) for i, (e, n) in enumerate(((e0, i0),) * 2 + ((e1, i1),) * 2)
    ]
    pulled, divisors = [], []
    for k, wv, h, l, g, s in ((0, wv0, h0, l0, g0, s0), (1, wv1, h1, l1, g1, s1)):
        gram, total = gram_of(("inner",), 16, *patches[k : k + 3], None, None, fars[k], wv, h, l, g)
        pulled.append(jnp.sum(total + pulled_in[k], axis=1, keepdims=True))
        divisors.append(start_newton(gram + gram_in[k], s))

    def body(_, carry):
        newton(s0, s1, False)
        return carry

    lax.fori_loop(0, ITERS - 2, body, 0)
    newton(s0, s1, True)
    for k, s in ((0, s0), (1, s1)):
        apply(s[1], pulled[k], divisors[k], patches[k + 1], out, 8 * k)


def analysis(edge, inner, grams, pulls, wv, pairs, *ends):
    outer = pairs[-1] == 7
    steps = len(pairs)
    start = (pairs[0] - 1) // 2

    def block(shift):
        return pl.BlockSpec((256, 8, 128), lambda i: (0, (start + i + shift) % 4, 0))

    def cells(shift):
        return pl.BlockSpec((1, 72, 128), lambda i: ((2 * (start + i) + 1 + shift) % 8, 0, 0))

    def held(width):
        return pl.BlockSpec((2, 256, width), lambda i: (start + i, 0, 0))

    args = [edge, edge, inner, inner, grams, pulls, wv, wv]
    specs = [block(0), block(1), block(0), block(1), held(256), held(128), cells(0), cells(1)]
    if outer:
        args += list(ends)
        specs += [whole(v.shape) for v in ends]
    return pl.pallas_call(
        functools.partial(analysis_kernel, pairs, outer),
        grid=(steps,),
        in_specs=specs,
        out_specs=pl.BlockSpec((256, 16, 128), lambda i: (0, i, 0)),
        out_shape=jax.ShapeDtypeStruct((256, 16 * steps, 128), F32),
        scratch_shapes=[pltpu.VMEM((256, 1024), BF16)] * 4 + [pltpu.VMEM((2, 256, 256), F32)] * 4,
        compiler_params=pltpu.CompilerParams(vmem_limit_bytes=58 * 1024 * 1024),
        cost_estimate=pl.CostEstimate(
            flops=steps * 12 * 10**9, bytes_accessed=steps * 6 * 2**20, transcendentals=0
        ),
        name="analysis",
    )(*args)


def shards(background, obs_cells, obs_counts, obs_widths, obs_values, obs_variances):
    axes = ("gx", "gy")
    gx, gy = lax.axis_size("gx"), lax.axis_size("gy")
    onward = [(i, i + 1) for i in range(gy - 1)]
    ring = [(i, (i + 1) % gx) for i in range(gx)]

    def exchange(x):
        return lax.all_to_all(x, axes, split_axis=0, concat_axis=0, tiled=True)

    def beside(pair):
        to_left, to_right = pair
        left = lax.ppermute(to_right, "gx", ring)
        return left, lax.ppermute(to_left, "gx", [(j, i) for i, j in ring])

    edge = exchange(pack(background, True).reshape(256, 32, 128))
    send = pack(background, False).reshape(256, 32, 128)
    wv = cell_sums(obs_cells[0], obs_counts[0], obs_widths[0], obs_values[0], obs_variances[0])
    tiles = edge.reshape(256, 4, 8, 128)
    up = tiles[:, :, 0:4].reshape(256, 16, 128)
    dn = tiles[:, :, 4:8].reshape(256, 16, 128)
    up, dn = lax.optimization_barrier((up, dn))
    above = lax.ppermute(dn, "gy", onward)
    below = lax.ppermute(up, "gy", [(j, i) for i, j in onward])
    inner = exchange(send)
    sides_e = beside(sides(edge, ("edge", "halo"), above, below))
    partial = early(edge, above, below, wv, 0, 3)
    sides_i = beside(sides(inner, ("inner",)))
    out = analysis(edge, inner, *partial, wv, FIRST)
    out, sides_e, sides_i = lax.optimization_barrier((out, sides_e, sides_i))
    results = [exchange(out)]
    partial = early(edge, above, below, wv, 3, 1, *sides_e, *partial)
    out = analysis(edge, inner, *partial, wv, SECOND, *sides_i)
    results.append(exchange(out))
    order = [[q % 8 for p in pairs for q in (p, p + 1)] for pairs in (FIRST, SECOND)]
    a, b = [r.reshape(4, 32, 2, r.shape[1], 128) for r in results]
    return unpack(a, b, order)


def solution(mesh):
    return jax.shard_map(
        shards,
        mesh=mesh,
        in_specs=(
            P(("gx", "gy"), None, None, None),
            P("gy", "gx", None),
            P("gy", "gx"),
            P("gy", "gx"),
            P("gy", "gx", None),
            P("gy", "gx", None),
        ),
        out_specs=P(("gx", "gy"), None, None, None),
        check_vma=False,
    )
```

```python
import functools

import jax
import jax.numpy as jnp
from jax import lax
from jax.experimental import pallas as pl
from jax.experimental.pallas import tpu as pltpu
from jax.sharding import PartitionSpec as P

F32 = jnp.float32
BF16 = jnp.bfloat16
ITERS = 5
FIRST, SECOND = (1, 3), (5, 7)


def lane_group(shape):
    return lax.broadcasted_iota(jnp.int32, shape, len(shape) - 1) // 16


def skew(tiles):
    group = lane_group(tiles[0].shape)
    for bit in (1, 2, 4):
        odd = (group & bit) != 0
        tiles = [jnp.where(odd, tiles[(k + bit) % 8], tiles[k]) for k in range(8)]
    return tiles


def edge_lanes():
    shape = (8, 128)
    low = lax.broadcasted_iota(jnp.int32, shape, 0) < 4
    return (lane_group(shape) % 2 == 0) == low


def pack_kernel(x_ref, o_ref, *, edge):
    first = edge_lanes()

    @pl.loop(0, o_ref.shape[1])
    def _(band):
        for member in range(2):
            for col in range(4):
                tiles = []
                for t in range(8):
                    rows = pl.ds(pl.multiple_of(16 * band + 8 * (t % 2), 8), 8)
                    tile = x_ref[member, t // 2, rows, 128 * col : 128 * col + 128]
                    tiles.append(pltpu.roll(tile, 16 * t, 1) if t else tile)
                tiles = skew(tiles)
                for i in range(4):
                    even, odd = tiles[(8 - 2 * i) % 8], tiles[7 - 2 * i]
                    merged = jnp.where(first, even, odd) if edge else jnp.where(first, odd, even)
                    o_ref[col, band, member, 8 * i : 8 * i + 8, :] = merged


def pack(x, edge, bands=8):
    return pl.pallas_call(
        functools.partial(pack_kernel, edge=edge),
        grid=(32 // bands,),
        in_specs=[pl.BlockSpec((2, 4, 16 * bands, 512), lambda i: (0, 0, i, 0))],
        out_specs=pl.BlockSpec((4, bands, 2, 32, 128), lambda i: (0, i, 0, 0, 0)),
        out_shape=jax.ShapeDtypeStruct((4, 32, 2, 32, 128), F32),
        cost_estimate=pl.CostEstimate(flops=10**10, bytes_accessed=12 * 2**20, transcendentals=0),
        name="pack_edge" if edge else "pack_inner",
    )(x)


def unpack_kernel(a_ref, b_ref, o_ref, *, order):
    place = {p: (a_ref, i) for i, p in enumerate(order[0])}
    place.update({p: (b_ref, i) for i, p in enumerate(order[1])})

    @pl.loop(0, a_ref.shape[1])
    def _(band):
        for member in range(2):
            for col in range(4):
                tiles = []
                for p in range(8):
                    ref, i = place[p]
                    tiles.append(ref[col, band, member, 8 * i : 8 * i + 8, :])
                tiles = skew(tiles)
                for t in range(8):
                    tile = tiles[(8 - t) % 8]
                    tile = pltpu.roll(tile, 128 - 16 * t, 1) if t else tile
                    rows = pl.ds(pl.multiple_of(16 * band + 8 * (t % 2), 8), 8)
                    o_ref[member, t // 2, rows, 128 * col : 128 * col + 128] = tile


def unpack(a, b, order, bands=8):
    na, nb = 8 * len(order[0]), 8 * len(order[1])
    return pl.pallas_call(
        functools.partial(unpack_kernel, order=order),
        grid=(32 // bands,),
        in_specs=[
            pl.BlockSpec((4, bands, 2, na, 128), lambda i: (0, i, 0, 0, 0)),
            pl.BlockSpec((4, bands, 2, nb, 128), lambda i: (0, i, 0, 0, 0)),
        ],
        out_specs=pl.BlockSpec((2, 4, 16 * bands, 512), lambda i: (0, 0, i, 0)),
        out_shape=jax.ShapeDtypeStruct((2, 4, 512, 512), F32),
        name="unpack",
    )(a, b)


def three_way(x):
    high = x.astype(BF16)
    rest = x - high.astype(F32)
    mid = rest.astype(BF16)
    return high, mid, (rest - mid.astype(F32)).astype(BF16)


def two_way(x):
    high = x.astype(BF16)
    return high, (x - high.astype(F32)).astype(BF16)


def cells_kernel(kc_ref, lane_ref, w_ref, v_ref, o_ref):
    kc = kc_ref[0]
    slots = kc.shape[1]
    row_hit = lax.broadcasted_iota(jnp.int32, (24, slots), 0) == kc
    lane_hit = lax.broadcasted_iota(jnp.int32, (128, slots), 0) == lane_ref[0]
    lane_hot = jnp.where(lane_hit, 1.0, 0.0).astype(BF16)
    both = jnp.concatenate(
        [jnp.where(row_hit, w_ref[0], 0.0), jnp.where(row_hit, v_ref[0], 0.0)], axis=0
    )
    total = jnp.zeros((48, 128), F32)
    for part in three_way(both):
        total = total + lax.dot_general(
            part, lane_hot, (((1,), (1,)), ((), ())), preferred_element_type=F32
        )
    w = total[:24]
    root = jnp.where(w > 0.0, jnp.sqrt(jnp.maximum(w, 1e-30)), 0.0)
    o_ref[0] = jnp.concatenate([total, root], axis=0)


def cell_sums(obs_cells, obs_counts, obs_widths, obs_values, obs_variances):
    number, slots = obs_cells.shape
    level = obs_cells // 576
    row = obs_cells // 24 % 24
    col = obs_cells % 24
    row_out = jnp.maximum(jnp.maximum(4 - row, row - 19), 0)
    col_out = jnp.maximum(jnp.maximum(4 - col, col - 19), 0)
    distance = jnp.maximum(row_out, col_out)
    slot = lax.broadcasted_iota(jnp.int32, obs_cells.shape, 1)
    usable = (slot < obs_counts[:, None]) & (distance <= obs_widths[:, None])
    relative = distance.astype(F32) / (obs_widths[:, None] + 1).astype(F32)
    w = jnp.where(usable, jnp.exp(-relative * relative) / obs_variances, 0.0)
    v = w * obs_values
    t = 2 * level + jnp.where((row >= 12) & (row < 20) | (row < 4), 1, 0)
    halo = (row < 4) | (row >= 20)
    inside = (row >= 8) & (row < 16)
    west, east = col < 4, col >= 20
    shift = jnp.where(west, -1, jnp.where(east, 1, 0))
    inner = jnp.where(west, 12 + col, jnp.where(east, col - 20, col - 4))
    p = lax.broadcasted_iota(jnp.int32, obs_cells.shape, 0)
    lane = 16 * ((t + p + shift + 8) % 8) + inner
    side = jnp.where(west | east, 1, 0)
    kc = row % 4 + jnp.where(inside, 16 + 4 * side, 8 * side + jnp.where(halo, 4, 0))
    spec = pl.BlockSpec((1, 1, slots), lambda i: (i, 0, 0))
    shape = (number, 1, slots)
    return pl.pallas_call(
        cells_kernel,
        grid=(number,),
        in_specs=[spec] * 4,
        out_specs=pl.BlockSpec((1, 72, 128), lambda i: (i, 0, 0)),
        out_shape=jax.ShapeDtypeStruct((number, 72, 128), F32),
        cost_estimate=pl.CostEstimate(flops=5 * 10**9, bytes_accessed=2**20, transcendentals=0),
        name="cells",
    )(kc.reshape(shape), lane.reshape(shape), w.reshape(shape), v.reshape(shape))


def take(ref, row):
    members, rows, lanes = ref.shape
    return ref.reshape(members * rows, lanes)[pl.ds(row, members, stride=rows), :]


def put(ref, row, value):
    members, rows, lanes = ref.shape
    ref.reshape(members * rows, lanes)[pl.ds(row, members, stride=rows), :] = value


def odd_rows(odd):
    return ((lane_group((1, 128)) - odd) & 1) == 1


def column(kind, q, patch, above, below):
    edge, inner, pair, odd = patch
    if kind == "edge":
        a, b = take(edge, q), take(edge, 4 + q)
    elif kind == "inner":
        a, b = take(inner, 4 + q), take(inner, q)
    else:
        a, b = take(below, 4 * pair + q), take(above, 4 * pair + q)
    return jnp.where(odd_rows(odd), b, a)


def sides_kernel(*refs, kinds):
    count = len(kinds)
    first_ref, last_ref = refs[:2]
    above, below = refs[2:4] if "halo" in kinds else (None, None)
    left_ref, right_ref = refs[-2:]
    within = lax.broadcasted_iota(jnp.int32, (1, 128), 1) % 16 // 4
    for j in range(count):
        left = right = None
        for i in range(4):
            f = column(kinds[j], i, (first_ref, first_ref, 0, 0), above, below)
            f = pltpu.roll(f, 4 * i, 1) if i else f
            l = column(kinds[j], i, (last_ref, last_ref, 3, 1), above, below)
            l = pltpu.roll(l, 128 - 4 * (3 - i), 1) if i < 3 else l
            left = f if left is None else jnp.where(within == i, f, left)
            right = l if right is None else jnp.where(within == i, l, right)
        left_ref[:, 128 * j : 128 * j + 128] = left
        right_ref[:, 128 * j : 128 * j + 128] = right


def whole(shape):
    return pl.BlockSpec(shape, lambda i: (0,) * len(shape))


def sides(x, kinds, *halo):
    width = 128 * len(kinds)
    return pl.pallas_call(
        functools.partial(sides_kernel, kinds=kinds),
        grid=(1,),
        in_specs=[
            pl.BlockSpec((256, 8, 128), lambda i: (0, 0, 0)),
            pl.BlockSpec((256, 8, 128), lambda i: (0, 3, 0)),
        ]
        + [whole((256, 16, 128))] * len(halo),
        out_specs=[whole((256, width))] * 2,
        out_shape=[jax.ShapeDtypeStruct((256, width), F32)] * 2,
        cost_estimate=pl.CostEstimate(flops=10**9, bytes_accessed=4 * 2**20, transcendentals=0),
        name="sides",
    )(x, x, *halo)


def dot(a, b):
    return jnp.dot(a, b, preferred_element_type=F32)


def product(a, b):
    (ah, al), (bh, bl) = a, b
    return dot(jnp.concatenate([ah, ah, al], axis=1), jnp.concatenate([bh, bl, bh], axis=0))


def gram_of(kinds, base, west, mine, east, above, below, far, wv, high_ref, low_ref, gram_ref):
    total = jnp.zeros((256, 128), F32)
    within = lax.broadcasted_iota(jnp.int32, (1, 128), 1) % 16
    place = 0
    for strip in (False, True):
        for j, kind in enumerate(kinds):
            for q in range(4):
                if not strip:
                    x = column(kind, q, mine, above, below)
                else:
                    l = column(kind, q, west, above, below)
                    r = column(kind, q, east, above, below)
                    if far is not None:
                        ref, from_west, outer = far
                        v = ref[:, 128 * j : 128 * j + 128]
                        if from_west:
                            v = pltpu.roll(v, 4 * (3 - q), 1) if q < 3 else v
                            l = jnp.where(outer, v, l)
                        else:
                            v = pltpu.roll(v, 128 - 4 * q, 1) if q else v
                            r = jnp.where(outer, v, r)
                    x = jnp.where(within < 8, r, l)
                c = base + place
                w = wv[0, c : c + 1, :]
                v = wv[0, 24 + c : 25 + c, :]
                root = wv[0, 48 + c : 49 + c, :]
                mean = jnp.sum(x, axis=0, keepdims=True) * (1.0 / 256)
                dev = x - mean
                total = total + dev * (v - w * mean)
                high, low = two_way(dev * root)
                high_ref[:, 128 * place : 128 * place + 128] = high
                low_ref[:, 128 * place : 128 * place + 128] = low
                place += 1
    nt = (((1,), (1,)), ((), ()))
    high, low = high_ref[:, : 128 * place], low_ref[:, : 128 * place]
    gram_ref[0] = lax.dot_general(high, high, nt, preferred_element_type=F32)
    gram_ref[1] = lax.dot_general(high, low, nt, preferred_element_type=F32)
    cross = gram_ref[1]
    return gram_ref[0] + (cross + cross.T), total


def early_kernel(start, *refs):
    e0, e1, above, below, wv0, wv1 = refs[:6]
    gram_out, pulled_out, h0, l0, h1, l1, g0, g1 = refs[-8:]
    pair = start + pl.program_id(0)
    patches = [(e, None, (pair + i // 2) % 4, i % 2) for i, e in enumerate((e0, e0, e1, e1))]
    fars = [(refs[7], False, True), (refs[6], True, True)] if start == 3 else [None, None]
    for k, wv, h, l, g in ((0, wv0, h0, l0, g0), (1, wv1, h1, l1, g1)):
        gram, total = gram_of(
            ("edge", "halo"), 0, *patches[k : k + 3], above, below, fars[k], wv, h, l, g
        )
        gram_out[k] = gram
        pulled_out[k] = total


def early(edge, above, below, wv, start, steps, *last):
    args = [edge, edge, above, below, wv, wv, *last]
    specs = [
        pl.BlockSpec((256, 8, 128), lambda i: (0, start + i, 0)),
        pl.BlockSpec((256, 8, 128), lambda i: (0, (start + i + 1) % 4, 0)),
        whole((256, 16, 128)),
        whole((256, 16, 128)),
        pl.BlockSpec((1, 72, 128), lambda i: (2 * (start + i) + 1, 0, 0)),
        pl.BlockSpec((1, 72, 128), lambda i: ((2 * (start + i) + 2) % 8, 0, 0)),
    ]
    if last:
        specs += [whole((256, 256))] * 2 + [pl.BlockSpec(memory_space=pl.ANY)] * 2
    return pl.pallas_call(
        functools.partial(early_kernel, start),
        grid=(steps,),
        in_specs=specs,
        out_specs=[
            pl.BlockSpec((2, 256, 256), lambda i: (start + i, 0, 0)),
            pl.BlockSpec((2, 256, 128), lambda i: (start + i, 0, 0)),
        ],
        out_shape=[
            jax.ShapeDtypeStruct((8, 256, 256), F32),
            jax.ShapeDtypeStruct((8, 256, 128), F32),
        ],
        input_output_aliases={8: 0, 9: 1} if last else {},
        scratch_shapes=[pltpu.VMEM((256, 2048), BF16)] * 4 + [pltpu.VMEM((2, 256, 256), F32)] * 2,
        compiler_params=pltpu.CompilerParams(vmem_limit_bytes=58 * 1024 * 1024),
        cost_estimate=pl.CostEstimate(
            flops=steps * 7 * 10**9, bytes_accessed=steps * 4 * 2**20, transcendentals=0
        ),
        name="early",
    )(*args)


def newton(s0, s1, last):
    row = lax.broadcasted_iota(jnp.int32, (256, 256), 0)
    col = lax.broadcasted_iota(jnp.int32, (256, 256), 1)
    eye = jnp.where(row == col, 1.5, 0.0)
    halves = [(two_way(s[0]), two_way(s[1])) for s in (s0, s1)]
    both = [product(inv, cur) for cur, inv in halves]
    factors = [two_way(eye - 0.5 * x) for x in both]
    if not last:
        for s, (cur, _), factor in zip((s0, s1), halves, factors):
            s[0] = product(cur, factor)
    for s, (_, inv), factor in zip((s0, s1), halves, factors):
        s[1] = product(factor, inv)


def start_newton(gram, s):
    squares = jnp.sum(jnp.sum(gram * gram, axis=0, keepdims=True), axis=1, keepdims=True)
    divisor = 255.0 + jnp.sqrt(jnp.maximum(squares, 1e-30))
    row = lax.broadcasted_iota(jnp.int32, (256, 256), 0)
    col = lax.broadcasted_iota(jnp.int32, (256, 256), 1)
    eye = row == col
    current = (gram + jnp.where(eye, 255.0, 0.0)) / divisor
    inverse = jnp.where(eye, 1.5, 0.0) - 0.5 * current
    s[0] = product(two_way(current), two_way(inverse))
    s[1] = inverse
    return divisor


def apply(inverse, pulled, divisor, mine, out, base):
    halfway = jnp.sum(inverse * pulled, axis=0, keepdims=True)
    weight = jnp.sum(inverse * halfway, axis=1, keepdims=True) / divisor
    zh, zl = two_way(inverse * jnp.sqrt(255.0 / divisor))
    z = jnp.concatenate([zh, zh, zl], axis=1)
    edge, inner, _, odd = mine
    for q in range(0, 8, 2):
        parts, bases = [], []
        for k in range(2):
            a, b = take(edge, q + k), take(inner, q + k)
            x = jnp.where(odd_rows(odd), b, a) if q < 4 else jnp.where(odd_rows(odd), a, b)
            centre = jnp.sum(x, axis=0, keepdims=True) * (1.0 / 256)
            dev = x - centre
            bases.append(centre + jnp.sum(dev * weight, axis=0, keepdims=True))
            parts.append(dev)
        dh, dl = two_way(jnp.concatenate(parts, axis=1))
        mixed = dot(z, jnp.concatenate([dh, dl, dh], axis=0))
        for k in range(2):
            put(out, base + q + k, mixed[:, 128 * k : 128 * k + 128] + bases[k])


def analysis_kernel(pairs, outer, *refs):
    e0, e1, i0, i1, gram_in, pulled_in, wv0, wv1 = refs[:8]
    refs = refs[8:]
    step = pl.program_id(0)
    pair = (pairs[0] - 1) // 2 + step
    fars = [None, None]
    if outer:
        fars = [(refs[1], False, pair == 3), (refs[0], True, pair == 3)]
        refs = refs[2:]
    out, h0, l0, h1, l1, g0, g1, s0, s1 = refs
    patches = [
        (e, n, (pair + i // 2) % 4, i % 2) for i, (e, n) in enumerate(((e0, i0),) * 2 + ((e1, i1),) * 2)
    ]
    pulled, divisors = [], []
    for k, wv, h, l, g, s in ((0, wv0, h0, l0, g0, s0), (1, wv1, h1, l1, g1, s1)):
        gram, total = gram_of(("inner",), 16, *patches[k : k + 3], None, None, fars[k], wv, h, l, g)
        pulled.append(jnp.sum(total + pulled_in[k], axis=1, keepdims=True))
        divisors.append(start_newton(gram + gram_in[k], s))

    def body(_, carry):
        newton(s0, s1, False)
        return carry

    lax.fori_loop(0, ITERS - 2, body, 0)
    newton(s0, s1, True)
    for k, s in ((0, s0), (1, s1)):
        apply(s[1], pulled[k], divisors[k], patches[k + 1], out, 8 * k)


def analysis(edge, inner, grams, pulls, wv, pairs, *ends):
    outer = pairs[-1] == 7
    steps = len(pairs)
    start = (pairs[0] - 1) // 2

    def block(shift):
        return pl.BlockSpec((256, 8, 128), lambda i: (0, (start + i + shift) % 4, 0))

    def cells(shift):
        return pl.BlockSpec((1, 72, 128), lambda i: ((2 * (start + i) + 1 + shift) % 8, 0, 0))

    def held(width):
        return pl.BlockSpec((2, 256, width), lambda i: (start + i, 0, 0))

    args = [edge, edge, inner, inner, grams, pulls, wv, wv]
    specs = [block(0), block(1), block(0), block(1), held(256), held(128), cells(0), cells(1)]
    if outer:
        args += list(ends)
        specs += [whole(v.shape) for v in ends]
    return pl.pallas_call(
        functools.partial(analysis_kernel, pairs, outer),
        grid=(steps,),
        in_specs=specs,
        out_specs=pl.BlockSpec((256, 16, 128), lambda i: (0, i, 0)),
        out_shape=jax.ShapeDtypeStruct((256, 16 * steps, 128), F32),
        scratch_shapes=[pltpu.VMEM((256, 1024), BF16)] * 4 + [pltpu.VMEM((2, 256, 256), F32)] * 4,
        compiler_params=pltpu.CompilerParams(vmem_limit_bytes=58 * 1024 * 1024),
        cost_estimate=pl.CostEstimate(
            flops=steps * 12 * 10**9, bytes_accessed=steps * 6 * 2**20, transcendentals=0
        ),
        name="analysis",
    )(*args)


def shards(background, obs_cells, obs_counts, obs_widths, obs_values, obs_variances):
    axes = ("gx", "gy")
    gx, gy = lax.axis_size("gx"), lax.axis_size("gy")
    onward = [(i, i + 1) for i in range(gy - 1)]
    ring = [(i, (i + 1) % gx) for i in range(gx)]

    def exchange(x):
        return lax.all_to_all(x, axes, split_axis=0, concat_axis=0, tiled=True)

    def beside(pair):
        to_left, to_right = pair
        left = lax.ppermute(to_right, "gx", ring)
        return left, lax.ppermute(to_left, "gx", [(j, i) for i, j in ring])

    edge = exchange(pack(background, True).reshape(256, 32, 128))
    send = pack(background, False).reshape(256, 32, 128)
    tiles = edge.reshape(256, 4, 8, 128)
    up = tiles[:, :, 0:4].reshape(256, 16, 128)
    dn = tiles[:, :, 4:8].reshape(256, 16, 128)
    up, dn, obs_cells, obs_counts, obs_widths = lax.optimization_barrier(
        (up, dn, obs_cells, obs_counts, obs_widths)
    )
    wv = cell_sums(obs_cells[0], obs_counts[0], obs_widths[0], obs_values[0], obs_variances[0])
    above = lax.ppermute(dn, "gy", onward)
    below = lax.ppermute(up, "gy", [(j, i) for i, j in onward])
    send, wv = lax.optimization_barrier((send, wv))
    inner = exchange(send)
    sides_e = beside(sides(edge, ("edge", "halo"), above, below))
    partial = early(edge, above, below, wv, 0, 3)
    sides_i = beside(sides(inner, ("inner",)))
    out = analysis(edge, inner, *partial, wv, FIRST)
    out, sides_e, sides_i = lax.optimization_barrier((out, sides_e, sides_i))
    results = [exchange(out)]
    partial = early(edge, above, below, wv, 3, 1, *sides_e, *partial)
    out = analysis(edge, inner, *partial, wv, SECOND, *sides_i)
    results.append(exchange(out))
    order = [[q % 8 for p in pairs for q in (p, p + 1)] for pairs in (FIRST, SECOND)]
    a, b = [r.reshape(4, 32, 2, r.shape[1], 128) for r in results]
    return unpack(a, b, order)


def solution(mesh):
    return jax.shard_map(
        shards,
        mesh=mesh,
        in_specs=(
            P(("gx", "gy"), None, None, None),
            P("gy", "gx", None),
            P("gy", "gx"),
            P("gy", "gx"),
            P("gy", "gx", None),
            P("gy", "gx", None),
        ),
        out_specs=P(("gx", "gy"), None, None, None),
        check_vma=False,
    )
```
